16 devices in a mesh: rep: 2 (over y, z), vocab: 8 (over x, core).
Axes of the slice: x: 4, y: 2, z: 1, core: 2. Of those that a mesh axis runs over, the one named last changes fastest.
The devices are a block of a 4x4x8 slice.
Arguments:
- hidden: bfloat16 [8192, 2304], P(('rep', 'vocab')), parts along dimension 0
- w_head: bfloat16 [256000, 2304], P('vocab')
- allowed_ids: int32 [4096], P('rep'), parts along dimension 0
- allowed_valid: int32 [4096], P('rep'), parts along dimension 0
- target_pos: int32 [8192], P(('rep', 'vocab')), parts along dimension 0
Outputs:
- output 1: float32 [8192, 2048], P(('rep', 'vocab')), parts along dimension 0
- output 2: float32 [8192], P(('rep', 'vocab')), parts along dimension 0
There are 2 independent parts. The reference program is written for one: setup_inputs(seed, part) draws one part's arguments, and reference() takes and returns one part's arrays. A program takes and returns all parts, laid end to end along the dimension named above; an argument that names none is the same for every part.
All inputs are finite; a program needn't handle non-finite values.
Results may differ from the reference program's by a relative error of at most 0.001.
Values are sent between devices in bfloat16 or wider.
A program may use at most 768 MiB of HBM per device.

```python
import jax
import jax.numpy as jnp
from jax import lax

VOCAB_SIZE = 256000
MODEL_DIM = 2304
LIST_LEN = 2048
BATCH_ROWS = 4096
SHARDS = 8
HEAD_BLOCKS = 128
INV_TEMP = 1.25


def draw_head(key_head):
    block_keys = jax.random.split(key_head, HEAD_BLOCKS)
    row_scale = MODEL_DIM ** -0.5

    def one_block(block_key):
        block_vals = jax.random.normal(block_key, (VOCAB_SIZE // HEAD_BLOCKS, MODEL_DIM), jnp.float32)
        return (block_vals * row_scale).astype(jnp.bfloat16)

    return lax.map(one_block, block_keys).reshape(VOCAB_SIZE, MODEL_DIM)


def draw_list(key_list):
    key_pair, key_move, key_offset, key_order, key_count, key_valid, key_target = jax.random.split(key_list, 7)
    per_shard = LIST_LEN // SHARDS
    slot_cap = 2 * per_shard
    vocab_local = VOCAB_SIZE // SHARDS
    shard_order = jax.random.permutation(key_pair, SHARDS)
    move_sizes = jax.random.randint(key_move, (SHARDS // 2,), 0, per_shard + 1).at[0].set(per_shard)
    shard_gain = jnp.zeros((SHARDS,), jnp.int32).at[shard_order[0::2]].set(move_sizes).at[shard_order[1::2]].set(-move_sizes)
    counts = per_shard + shard_gain
    offset_keys = jax.random.split(key_offset, SHARDS)
    offsets = jax.vmap(lambda one_key: jax.random.permutation(one_key, vocab_local)[:slot_cap])(offset_keys)
    candidates = jnp.arange(SHARDS, dtype=jnp.int32)[:, None] * vocab_local + offsets
    keep_slot = jnp.arange(slot_cap)[None, :] < counts[:, None]
    sort_key = jnp.where(keep_slot, 0, 1) * (SHARDS * slot_cap) + jnp.arange(SHARDS * slot_cap).reshape(SHARDS, slot_cap)
    chosen = jnp.argsort(sort_key.reshape(-1))[:LIST_LEN]
    grouped = candidates.reshape(-1)[chosen]
    allowed_ids = grouped[jax.random.permutation(key_order, LIST_LEN)].astype(jnp.int32)
    valid_count = jax.random.randint(key_count, (), LIST_LEN // 2, LIST_LEN + 1)
    valid_perm = jax.random.permutation(key_valid, LIST_LEN)
    allowed_valid = (valid_perm < valid_count).astype(jnp.int32)
    inverse = jnp.argsort(valid_perm)
    pick_rank = jax.random.randint(key_target, (BATCH_ROWS,), 0, valid_count)
    target_pos = inverse[pick_rank].astype(jnp.int32)
    return allowed_ids, allowed_valid, target_pos


def setup_inputs(seed: int = 0, part: int = 0) -> dict:
    root_key = jax.random.key(seed)
    key_head, key_groups = jax.random.split(root_key)
    key_part = jax.random.fold_in(key_groups, part)
    key_hidden, key_list = jax.random.split(key_part)
    hidden = jax.random.normal(key_hidden, (BATCH_ROWS, MODEL_DIM), jnp.float32).astype(jnp.bfloat16)
    allowed_ids, allowed_valid, target_pos = draw_list(key_list)
    return dict(hidden=hidden, w_head=draw_head(key_head), allowed_ids=allowed_ids, allowed_valid=allowed_valid, target_pos=target_pos)


def reference(hidden, w_head, allowed_ids, allowed_valid, target_pos):
    head_rows = jnp.take(w_head, allowed_ids, axis=0)
    scores = jnp.dot(hidden, head_rows.T, preferred_element_type=jnp.float32) * INV_TEMP
    keep_mask = (allowed_valid > 0)[None, :]
    masked = jnp.where(keep_mask, scores, -jnp.inf)
    log_norm = jax.nn.logsumexp(masked, axis=1)
    token_probs = jnp.where(keep_mask, jnp.exp(masked - log_norm[:, None]), 0.0)
    picked = jnp.take_along_axis(scores, target_pos[:, None], axis=1)[:, 0]
    return token_probs, picked - log_norm
```

```python
import jax
import jax.numpy as jnp
from jax import lax
from jax.sharding import PartitionSpec as P

INV_TEMP = 1.25


def solution(mesh):

    def device_step(hidden, w_head, allowed_ids, allowed_valid, target_pos):
        my_index = lax.axis_index('vocab')
        vocab_local = w_head.shape[0]
        local_idx = allowed_ids - my_index * vocab_local
        mine = (local_idx >= 0) & (local_idx < vocab_local)
        rows = jnp.take(w_head, jnp.clip(local_idx, 0, vocab_local - 1), axis=0)
        rows = jnp.where(mine[:, None], rows, jnp.zeros((), rows.dtype))
        part = lax.psum_scatter(rows, 'vocab', scatter_dimension=0, tiled=True)
        rows = lax.all_gather(part, 'vocab', axis=0, tiled=True)
        scores = lax.dot_general(hidden, rows, (((1,), (1,)), ((), ())), preferred_element_type=jnp.float32) * INV_TEMP
        keep_mask = (allowed_valid > 0)[None, :]
        masked = jnp.where(keep_mask, scores, -jnp.inf)
        log_norm = jax.nn.logsumexp(masked, axis=1)
        token_probs = jnp.where(keep_mask, jnp.exp(masked - log_norm[:, None]), 0.0)
        lane = lax.broadcasted_iota(jnp.int32, scores.shape, 1)
        picked = jnp.sum(jnp.where(lane == target_pos[:, None], scores, 0.0), axis=1)
        return token_probs, picked - log_norm

    row_spec = P(('rep', 'vocab'))
    mat_spec = P(('rep', 'vocab'), None)
    return jax.shard_map(device_step, mesh=mesh, in_specs=(mat_spec, P('vocab', None), P('rep'), P('rep'), row_spec), out_specs=(mat_spec, row_spec), check_vma=False)
```

```python
import functools

import jax
import jax.numpy as jnp
from jax import lax
from jax.experimental import pallas as pl
from jax.experimental.pallas import tpu as pltpu
from jax.sharding import PartitionSpec as P

INV_TEMP = 1.25
MESH = pl.DeviceIdType.MESH
CHUNK = 64
LAG = 2
GATHER = 32
PACK = 8
GROUP = 256
CUT = 384


def gather_kernel(shards, base_ref, sid_ref, w_ref, gbuf_ref, stage, pick, outb, in_sem, out_sem):
    v = lax.axis_index('vocab')
    vocab_local = w_ref.shape[0]
    half = gbuf_ref.shape[1]
    chip = v // 2

    def span(k):
        first = base_ref[k * (shards + 1) + v]
        count = base_ref[k * (shards + 1) + v + 1] - first
        slot0 = first - base_ref[k * (shards + 1) + 2 * chip]
        block0 = slot0 // GATHER
        blocks = jnp.where(count > 0, (slot0 + count + GATHER - 1) // GATHER - block0, 0)
        return first, count, slot0, block0, blocks

    spans = [span(0), span(1)]
    total = spans[0][4] + spans[1][4]

    def where_is(t):
        second = t >= spans[0][4]
        first, count, slot0, block0 = [jnp.where(second, spans[1][i], spans[0][i]) for i in range(4)]
        k = jnp.where(second, 1, 0)
        block = block0 + jnp.where(second, t - spans[0][4], t)
        lo = jnp.maximum(slot0 - block * GATHER, 0)
        hi = jnp.minimum(slot0 + count - block * GATHER, GATHER)
        src = k * half + first + block * GATHER - slot0
        return k, block, lo, hi, src

    def row_copy(group, s, b):
        return pltpu.make_async_copy(
            w_ref.at[pl.ds(pl.multiple_of(group * PACK, PACK), PACK), :],
            stage.at[b, pl.ds(pl.multiple_of(s * PACK, PACK), PACK), :],
            in_sem.at[b])

    def out_copy(t, b):
        k, block, _, _, _ = where_is(t)
        return pltpu.make_async_copy(
            outb.at[b], gbuf_ref.at[k, pl.ds(pl.multiple_of(block * GATHER, GATHER), GATHER), :], out_sem.at[b])

    lane = lax.broadcasted_iota(jnp.int32, (1, GATHER * PACK), 1)

    def issue(t, b):
        _, _, lo, hi, src = where_is(t)
        pick[b] = jnp.zeros((GATHER, GATHER * PACK), jnp.float32)

        def one(s, carry):
            local = sid_ref[src + s] - v * vocab_local
            group = local // PACK
            row_copy(group, s, b).start()
            pick[b, pl.ds(s, 1), :] = jnp.where(lane == s * PACK + local - group * PACK, 1.0, 0.0)
            return carry

        lax.fori_loop(lo, hi, one, 0)

    stage[...] = jnp.zeros_like(stage)

    @pl.when(total > 0)
    def _():
        issue(0, 0)

    def step(t, carry):
        b = lax.rem(t, 2)

        @pl.when(t + 1 < total)
        def _():
            issue(t + 1, 1 - b)

        _, _, lo, hi, _ = where_is(t)

        def one(s, c):
            row_copy(0, s, b).wait()
            return c

        lax.fori_loop(lo, hi, one, 0)

        @pl.when(t >= 2)
        def _():
            out_copy(t - 2, b).wait()

        outb[b] = jnp.dot(pick[b].astype(jnp.bfloat16), stage[b], preferred_element_type=jnp.float32).astype(jnp.bfloat16)
        out_copy(t, b).start()
        return carry

    lax.fori_loop(0, total, step, 0)

    @pl.when(total >= 2)
    def _():
        out_copy(total - 2, lax.rem(total, 2)).wait()

    @pl.when(total >= 1)
    def _():
        out_copy(total - 1, lax.rem(total + 1, 2)).wait()


def ring_kernel(shards, base_ref, rank_ref, hidden_ref, gbuf_ref, out_ref,
                hid, mine, other, land, merged, theirs, slot_of, shift,
                hid_sem, mine_sem, other_send, other_recv, ring_send, ring_recv, pair_send, pair_recv):
    chips = shards // 2
    half = gbuf_ref.shape[1]
    lag_rows = LAG * CHUNK
    n_own = half // CHUNK
    n_wire = n_own + (chips - 2) * LAG
    n_all = n_own + (chips - 1) * LAG
    max_delay = half // CHUNK + 1
    depth = mine.shape[1]
    v = lax.axis_index('vocab')
    core = lax.rem(v, 2)
    chip = v // 2
    partner = chip * 2 + 1 - core
    ahead = lax.rem(chip + 2 * core - 1 + chips, chips) * 2 + core
    behind = lax.rem(chip - 2 * core + 1 + chips, chips) * 2 + core

    barrier = pltpu.get_barrier_semaphore()
    for peer in (partner, ahead, behind):
        pl.semaphore_signal(barrier, inc=1, device_id={'vocab': peer}, device_id_type=MESH)

    def rows(e, n=CHUNK):
        return pl.ds(pl.multiple_of(e * CHUNK, CHUNK), n)

    hid_copy = pltpu.make_async_copy(hidden_ref, hid, hid_sem)

    def mine_copy(e):
        return pltpu.make_async_copy(gbuf_ref.at[core, rows(e), :], mine.at[rows(e), :], mine_sem.at[e])

    def other_copy(e):
        return pltpu.make_async_remote_copy(
            src_ref=gbuf_ref.at[1 - core, rows(e), :], dst_ref=other.at[rows(e), :],
            send_sem=other_send.at[e], recv_sem=other_recv.at[e], device_id={'vocab': partner}, device_id_type=MESH)

    def ring_copy(e):
        return pltpu.make_async_remote_copy(
            src_ref=merged.at[rows(e), :], dst_ref=land.at[rows(e), :],
            send_sem=ring_send.at[e], recv_sem=ring_recv.at[e], device_id={'vocab': ahead}, device_id_type=MESH)

    def pair_copy(e):
        return pltpu.make_async_remote_copy(
            src_ref=merged.at[rows(e), :], dst_ref=theirs.at[rows(e), :],
            send_sem=pair_send.at[e], recv_sem=pair_recv.at[e], device_id={'vocab': partner}, device_id_type=MESH)

    def start_mine(e, c):
        mine_copy(e).start()
        return c

    lax.fori_loop(0, n_own, start_mine, 0)
    hid_copy.start()

    def base(k, w):
        return base_ref[k * (shards + 1) + w]

    for k in range(2):
        rank = rank_ref[k]
        slots = jnp.zeros_like(rank)
        passed = jnp.int32(0)
        for hop in range(chips):
            owner = lax.rem(chip - (2 * k - 1) * hop + chips, chips)
            low, high = base(k, 2 * owner), base(k, 2 * owner + 2)
            slots += jnp.where((rank >= low) & (rank < high), rank + (passed - low), 0)
            passed += jnp.maximum(high - low, lag_rows)
        slot_of[k] = slots
    out_ref[...] = jnp.zeros_like(out_ref)

    pl.semaphore_wait(barrier, 3)
    ahead_of_use = 3
    for e in range(ahead_of_use):
        other_copy(e).start()

    chip_low = base(core, 2 * chip)
    own_pad = jnp.maximum(base(core, 2 * chip + 2) - chip_low, lag_rows)
    delay = (own_pad + CHUNK - 1) // CHUNK
    row = lax.broadcasted_iota(jnp.int32, (CHUNK, 2 * CHUNK), 0)
    col = lax.broadcasted_iota(jnp.int32, (CHUNK, 2 * CHUNK), 1)
    shift[...] = jnp.where(col == row + delay * CHUNK - own_pad, 1.0, 0.0).astype(jnp.bfloat16)
    mine_low = base(core, v) - chip_low
    mine_high = base(core, v + 1) - chip_low
    other_low = base(core, partner) - chip_low
    other_high = base(core, partner + 1) - chip_low

    def score(k, src, q, slots):
        part = src[pl.ds(pl.multiple_of(q * GROUP, GROUP), slots), :]
        s = lax.dot_general(hid[...], part, (((1,), (1,)), ((), ())), preferred_element_type=jnp.float32) * INV_TEMP
        top = s.astype(jnp.bfloat16)
        rest = s - top.astype(jnp.float32)
        mid = rest.astype(jnp.bfloat16)
        low = (rest - mid.astype(jnp.float32)).astype(jnp.bfloat16)
        slot = lax.broadcasted_iota(jnp.int32, (slots, half), 0) + q * GROUP
        place = jnp.where(slot == slot_of[k], 1.0, 0.0).astype(jnp.bfloat16)
        cols = pl.ds(pl.multiple_of(k * half, half), half)
        moved = (jnp.dot(top, place, preferred_element_type=jnp.float32)
                 + jnp.dot(mid, place, preferred_element_type=jnp.float32)
                 + jnp.dot(low, place, preferred_element_type=jnp.float32))
        out_ref[:, cols] = out_ref[:, cols] + moved

    per_group = GROUP // CHUNK

    def wait_theirs(first, count):
        def one(e, c):
            pair_copy(e).wait_recv()
            return c
        lax.fori_loop(first, first + count, one, 0)

    def step(e, carry):
        @pl.when(e + ahead_of_use < n_own)
        def _():
            other_copy(e + ahead_of_use).start()

        @pl.when(e < n_own)
        def _():
            mine_copy(e).wait()
            other_copy(e).wait_recv()

        @pl.when(e >= LAG)
        def _():
            ring_copy(e - LAG).wait_recv()

        slot = lax.broadcasted_iota(jnp.int32, (CHUNK, 1), 0) + e * CHUNK
        is_mine = (slot >= mine_low) & (slot < mine_high)
        is_other = (slot >= other_low) & (slot < other_high)
        e_own = jnp.minimum(e, n_own - 1)
        zero = jnp.zeros((), jnp.float32)
        for cut in range(depth // CUT):
            cols = pl.ds(cut * CUT, CUT)

            def pick(c, acc):
                part = land[rows(c), cols]
                return jnp.where(c == e - delay, part, acc[0]), jnp.where(c == e - delay + 1, part, acc[1])

            empty = jnp.zeros((CHUNK, CUT), land.dtype)
            first, second = lax.fori_loop(jnp.maximum(e - max_delay, 0), e - LAG + 1, pick, (empty, empty))
            forward = jnp.dot(shift[...], jnp.concatenate([first, second], axis=0), preferred_element_type=jnp.float32)
            from_mine = jnp.where(is_mine, mine[rows(e_own), cols].astype(jnp.float32), zero)
            from_other = jnp.where(is_other, other[rows(e_own), cols].astype(jnp.float32), zero)
            merged[rows(e), cols] = (from_mine + from_other + forward).astype(jnp.bfloat16)

        @pl.when(e < n_wire)
        def _():
            ring_copy(e).start()

        pair_copy(e).start()

        q = e // per_group - 1

        @pl.when((q >= 0) & (lax.rem(e, per_group) == 0))
        def _():
            @pl.when(q == 0)
            def _():
                hid_copy.wait()

            score(core, merged, q, GROUP)

        @pl.when((q >= 0) & (lax.rem(e, per_group) == per_group // 2))
        def _():
            wait_theirs(q * per_group, per_group)
            score(1 - core, theirs, q, GROUP)

        return carry

    lax.fori_loop(0, n_all, step, 0)

    own_done = 0
    their_done = 0
    for e in range(n_all):
        if e // per_group >= 1 and e % per_group == 0:
            own_done = e // per_group
        if e // per_group >= 1 and e % per_group == per_group // 2:
            their_done = e // per_group
    for q in range(own_done, pl.cdiv(n_all, per_group)):
        score(core, merged, q, min(GROUP, n_all * CHUNK - q * GROUP))
    for q in range(their_done, pl.cdiv(n_all, per_group)):
        count = min(per_group, n_all - q * per_group)
        wait_theirs(q * per_group, count)
        score(1 - core, theirs, q, count * CHUNK)

    def finish(e, c):
        @pl.when(e < n_own)
        def _():
            other_copy(e).wait_send()

        @pl.when(e < n_wire)
        def _():
            ring_copy(e).wait_send()

        pair_copy(e).wait_send()
        return c

    lax.fori_loop(0, n_all, finish, 0)


def softmax_kernel(s_ref, valid_ref, target_ref, probs_ref, logp_ref):
    s = s_ref[...]
    keep = valid_ref[...] > 0
    masked = jnp.where(keep, s, -jnp.inf)
    top = jnp.max(masked, axis=1, keepdims=True)
    lse = jnp.log(jnp.sum(jnp.exp(masked - top), axis=1, keepdims=True)) + top
    probs_ref[...] = jnp.where(keep, jnp.exp(masked - lse), 0.0)
    lane = lax.broadcasted_iota(jnp.int32, s.shape, 1)
    picked = jnp.sum(jnp.where(lane == target_ref[...], s, 0.0), axis=1, keepdims=True)
    logp_ref[...] = picked - lse


def solution(mesh):
    shards = mesh.shape['vocab']

    def device_step(hidden, w_head, allowed_ids, allowed_valid, target_pos):
        list_len = allowed_ids.shape[0]
        half = list_len // 2
        vocab_local, depth = w_head.shape
        rows_dev = hidden.shape[0]
        chips = shards // 2
        ids = allowed_ids.reshape(2, half)
        rank = jnp.sum((ids[:, :, None] < ids[:, None, :]).astype(jnp.int32), axis=1)
        at = lax.broadcasted_iota(jnp.int32, (2, half, half), 1)
        sorted_ids = jnp.sum(jnp.where(rank[:, None, :] == at, ids[:, None, :], 0), axis=2)
        edges = lax.broadcasted_iota(jnp.int32, (2, shards + 1, half), 1) * vocab_local
        base = jnp.sum((ids[:, None, :] < edges).astype(jnp.int32), axis=2).reshape(-1)

        gbuf = pl.pallas_call(
            functools.partial(gather_kernel, shards),
            out_shape=jax.ShapeDtypeStruct((2, half, depth), w_head.dtype),
            in_specs=[pl.BlockSpec(memory_space=pltpu.SMEM), pl.BlockSpec(memory_space=pltpu.SMEM), pl.BlockSpec(memory_space=pl.ANY)],
            out_specs=pl.BlockSpec(memory_space=pl.ANY),
            scratch_shapes=[
                pltpu.VMEM((2, GATHER * PACK, depth), w_head.dtype),
                pltpu.VMEM((2, GATHER, GATHER * PACK), jnp.float32),
                pltpu.VMEM((2, GATHER, depth), w_head.dtype),
                pltpu.SemaphoreType.DMA((2,)),
                pltpu.SemaphoreType.DMA((2,)),
            ],
            name='gather_rows',
        )(base, sorted_ids.reshape(-1), w_head)

        n_own = half // CHUNK
        n_wire = n_own + (chips - 2) * LAG
        n_all = n_own + (chips - 1) * LAG
        scores = pl.pallas_call(
            functools.partial(ring_kernel, shards),
            out_shape=jax.ShapeDtypeStruct((rows_dev, list_len), jnp.float32),
            in_specs=[pl.BlockSpec(memory_space=pltpu.SMEM), pl.BlockSpec(memory_space=pltpu.VMEM),
                      pl.BlockSpec(memory_space=pl.ANY), pl.BlockSpec(memory_space=pl.ANY)],
            out_specs=pl.BlockSpec(memory_space=pltpu.VMEM),
            scratch_shapes=[
                pltpu.VMEM((rows_dev, depth), hidden.dtype),
                pltpu.VMEM((half, depth), w_head.dtype),
                pltpu.VMEM((half, depth), w_head.dtype),
                pltpu.VMEM((n_wire * CHUNK, depth), w_head.dtype),
                pltpu.VMEM((n_all * CHUNK, depth), w_head.dtype),
                pltpu.VMEM((n_all * CHUNK, depth), w_head.dtype),
                pltpu.VMEM((2, 1, half), jnp.int32),
                pltpu.VMEM((CHUNK, 2 * CHUNK), jnp.bfloat16),
                pltpu.SemaphoreType.DMA,
                pltpu.SemaphoreType.DMA((n_own,)),
                pltpu.SemaphoreType.DMA((n_own,)),
                pltpu.SemaphoreType.DMA((n_own,)),
                pltpu.SemaphoreType.DMA((n_wire,)),
                pltpu.SemaphoreType.DMA((n_wire,)),
                pltpu.SemaphoreType.DMA((n_all,)),
                pltpu.SemaphoreType.DMA((n_all,)),
            ],
            compiler_params=pltpu.CompilerParams(collective_id=0, has_side_effects=True, vmem_limit_bytes=62 * 1024 * 1024),
            name='ring_scores',
        )(base, rank.reshape(2, 1, half), hidden, gbuf)

        tile = 128
        probs, logp = pl.pallas_call(
            softmax_kernel,
            grid=(rows_dev // tile,),
            out_shape=[jax.ShapeDtypeStruct((rows_dev, list_len), jnp.float32), jax.ShapeDtypeStruct((rows_dev, 1), jnp.float32)],
            in_specs=[pl.BlockSpec((tile, list_len), lambda i: (i, 0)), pl.BlockSpec((1, list_len), lambda i: (0, 0)),
                      pl.BlockSpec((tile, 1), lambda i: (i, 0))],
            out_specs=[pl.BlockSpec((tile, list_len), lambda i: (i, 0)), pl.BlockSpec((tile, 1), lambda i: (i, 0))],
            name='softmax',
        )(scores, allowed_valid.reshape(1, list_len), target_pos.reshape(rows_dev, 1))
        return probs, logp.reshape(rows_dev)

    row_spec = P(('rep', 'vocab'))
    mat_spec = P(('rep', 'vocab'), None)
    return jax.shard_map(device_step, mesh=mesh, in_specs=(mat_spec, P('vocab', None), P('rep'), P('rep'), row_spec), out_specs=(mat_spec, row_spec), check_vma=False)
```

```python
import functools

import jax
import jax.numpy as jnp
from jax import lax
from jax.experimental import pallas as pl
from jax.experimental.pallas import tpu as pltpu
from jax.sharding import PartitionSpec as P

INV_TEMP = 1.25
MESH = pl.DeviceIdType.MESH
CHUNK = 64
LAG = 2
GATHER = 32
PACK_BITS = 3
PACK = 1 << PACK_BITS
PIECES = 2
CUT = 768


def gather_kernel(base_ref, sid_ref, w_ref, gbuf_ref, stage, pick, outb, in_sem, out_sem):
    v = lax.axis_index('vocab')
    vocab_local = w_ref.shape[0]
    half = gbuf_ref.shape[1]
    chip = v // 2

    def span(k):
        first = base_ref[k, v]
        count = base_ref[k, v + 1] - first
        slot0 = first - base_ref[k, 2 * chip]
        block0 = slot0 // GATHER
        blocks = jnp.where(count > 0, (slot0 + count + GATHER - 1) // GATHER - block0, 0)
        return first, count, slot0, block0, blocks

    spans = [span(0), span(1)]
    total = spans[0][4] + spans[1][4]

    def where_is(t):
        second = t >= spans[0][4]
        first, count, slot0, block0 = [jnp.where(second, spans[1][i], spans[0][i]) for i in range(4)]
        k = jnp.where(second, 1, 0)
        block = block0 + jnp.where(second, t - spans[0][4], t)
        lo = jnp.maximum(slot0 - block * GATHER, 0)
        last = jnp.minimum(slot0 + count - block * GATHER, GATHER) - 1
        src = first + block * GATHER - slot0
        return k, block, lo, last, src

    def row_copy(group, s, b):
        return pltpu.make_async_copy(
            w_ref.at[pl.ds(pl.multiple_of(group * PACK, PACK), PACK), :],
            stage.at[b, pl.ds(pl.multiple_of(s * PACK, PACK), PACK), :],
            in_sem.at[b])

    def out_copy(t, b):
        k, block, _, _, _ = where_is(t)
        return pltpu.make_async_copy(
            outb.at[b], gbuf_ref.at[k, pl.ds(pl.multiple_of(block * GATHER, GATHER), GATHER), :], out_sem.at[b])

    lane = lax.broadcasted_iota(jnp.int32, (1, GATHER * PACK), 1)

    def issue(t, b):
        k, first, last, src = where_is(t)[0], *where_is(t)[2:]
        for s in range(GATHER):
            local = sid_ref[k, src + jnp.clip(s, first, last)] - v * vocab_local
            group = lax.shift_right_logical(local, PACK_BITS)
            row_copy(group, s, b).start()
            pick[b, pl.ds(s, 1), :] = jnp.where(lane == s * PACK + (local & (PACK - 1)), 1.0, 0.0)

    @pl.when(total > 0)
    def _():
        issue(0, 0)

    def step(t, carry):
        b = lax.rem(t, 2)

        @pl.when(t + 1 < total)
        def _():
            issue(t + 1, 1 - b)

        pltpu.make_async_copy(w_ref.at[pl.ds(0, GATHER * PACK), :], stage.at[b], in_sem.at[b]).wait()

        @pl.when(t >= 2)
        def _():
            out_copy(t - 2, b).wait()

        outb[b] = jnp.dot(pick[b].astype(jnp.bfloat16), stage[b], preferred_element_type=jnp.float32).astype(jnp.bfloat16)
        out_copy(t, b).start()
        return carry

    lax.fori_loop(0, total, step, 0)

    @pl.when(total >= 2)
    def _():
        out_copy(total - 2, lax.rem(total, 2)).wait()

    @pl.when(total >= 1)
    def _():
        out_copy(total - 1, lax.rem(total + 1, 2)).wait()


def ring_kernel(shards, base_ref, rank_ref, hidden_ref, gbuf_ref, out_ref,
                hid, mine, other, land, merged, theirs, slot_of, shift, older, newer,
                hid_sem, mine_sem, other_send, other_recv, ring_send, ring_recv, pair_send, pair_recv):
    chips = shards // 2
    half = gbuf_ref.shape[1]
    lag_rows = LAG * CHUNK
    n_own = half // CHUNK
    n_wire = n_own + (chips - 2) * LAG
    n_all = n_own + (chips - 1) * LAG
    max_delay = half // CHUNK + 1
    depth = mine.shape[1]
    v = lax.axis_index('vocab')
    core = lax.rem(v, 2)
    chip = v // 2
    partner = chip * 2 + 1 - core
    ahead = lax.rem(chip + 2 * core - 1 + chips, chips) * 2 + core
    behind = lax.rem(chip - 2 * core + 1 + chips, chips) * 2 + core

    barrier = pltpu.get_barrier_semaphore()
    for peer in (partner, ahead, behind):
        pl.semaphore_signal(barrier, inc=1, device_id={'vocab': peer}, device_id_type=MESH)

    def rows(e, n=CHUNK):
        return pl.ds(pl.multiple_of(e * CHUNK, CHUNK), n)

    hid_copy = pltpu.make_async_copy(hidden_ref, hid, hid_sem)

    def mine_copy(e):
        return pltpu.make_async_copy(gbuf_ref.at[core, rows(e), :], mine.at[rows(e), :], mine_sem.at[e])

    def other_copy(e):
        return pltpu.make_async_remote_copy(
            src_ref=gbuf_ref.at[1 - core, rows(e), :], dst_ref=other.at[rows(e), :],
            send_sem=other_send.at[e], recv_sem=other_recv.at[e], device_id={'vocab': partner}, device_id_type=MESH)

    def ring_copy(e):
        return pltpu.make_async_remote_copy(
            src_ref=merged.at[rows(e), :], dst_ref=land.at[rows(e), :],
            send_sem=ring_send.at[e], recv_sem=ring_recv.at[e], device_id={'vocab': ahead}, device_id_type=MESH)

    def pair_copy(e):
        return pltpu.make_async_remote_copy(
            src_ref=merged.at[rows(e), :], dst_ref=theirs.at[rows(e), :],
            send_sem=pair_send.at[e], recv_sem=pair_recv.at[e], device_id={'vocab': partner}, device_id_type=MESH)

    def start_mine(e, c):
        mine_copy(e).start()
        return c

    lax.fori_loop(0, n_own, start_mine, 0)
    hid_copy.start()

    def base(k, w):
        return base_ref[k, w]

    pl.semaphore_wait(barrier, 3)
    ahead_of_use = 3
    for e in range(ahead_of_use):
        other_copy(e).start()

    for k in range(2):
        rank = rank_ref[pl.ds(k, 1), :]
        slots = jnp.zeros_like(rank)
        passed = jnp.int32(0)
        for hop in range(chips):
            owner = lax.rem(chip - (2 * k - 1) * hop + chips, chips)
            low, high = base(k, 2 * owner), base(k, 2 * owner + 2)
            slots += jnp.where((rank >= low) & (rank < high), rank + (passed - low), 0)
            passed += jnp.maximum(high - low, lag_rows)
        slot_of[k] = slots
    older[...] = jnp.zeros_like(older)
    newer[...] = jnp.zeros_like(newer)

    chip_low = base(core, 2 * chip)
    own_pad = jnp.maximum(base(core, 2 * chip + 2) - chip_low, lag_rows)
    delay = (own_pad + CHUNK - 1) // CHUNK
    row = lax.broadcasted_iota(jnp.int32, (CHUNK, 2 * CHUNK), 0)
    col = lax.broadcasted_iota(jnp.int32, (CHUNK, 2 * CHUNK), 1)
    shift[...] = jnp.where(col == row + delay * CHUNK - own_pad, 1.0, 0.0).astype(jnp.bfloat16)
    mine_low = base(core, v) - chip_low
    mine_high = base(core, v + 1) - chip_low
    other_low = base(core, partner) - chip_low
    other_high = base(core, partner + 1) - chip_low

    pair = 2 * CHUNK

    def move(k, s, p, at, n):
        top = s.astype(jnp.bfloat16)
        rest = s - top.astype(jnp.float32)
        mid = rest.astype(jnp.bfloat16)
        low = (rest - mid.astype(jnp.float32)).astype(jnp.bfloat16)
        slot = lax.broadcasted_iota(jnp.int32, (pair, half), 0) + p * pair
        place = jnp.where(slot == slot_of[k], 1.0, 0.0).astype(jnp.bfloat16)
        moved = jnp.dot(jnp.concatenate([top, mid, low], axis=1), jnp.concatenate([place] * 3, axis=0),
                        preferred_element_type=jnp.float32)
        spot = (pl.ds(at, n), pl.ds(pl.multiple_of(k * half, half), half))
        out_ref[spot] = out_ref[spot] + moved

    def pair_rows(p):
        return pl.ds(pl.multiple_of(p * pair, pair), pair)

    def against(at, n, part):
        return lax.dot_general(hid[pl.ds(at, n), :], part, (((1,), (1,)), ((), ())), preferred_element_type=jnp.float32) * INV_TEMP

    n_rows = hid.shape[0]

    def score(p, at, n):
        s = against(at, n, jnp.concatenate([merged[pair_rows(p), :], theirs[pair_rows(p), :]], axis=0))
        move(core, s[:, :pair], p, at, n)
        move(1 - core, s[:, pair:], p, at, n)

    def step(e, carry):
        @pl.when(e + ahead_of_use < n_own)
        def _():
            other_copy(e + ahead_of_use).start()

        @pl.when(e < n_own)
        def _():
            mine_copy(e).wait()
            other_copy(e).wait_recv()

        @pl.when(e >= LAG)
        def _():
            ring_copy(e - LAG).wait_recv()
            for cut in range(depth // CUT):
                cols = pl.ds(cut * CUT, CUT)
                fresh = land[rows(e - LAG), cols]
                older[:, cols] = jnp.where(delay == LAG, fresh, older[:, cols])
                newer[:, cols] = jnp.where(delay == LAG + 1, fresh, newer[:, cols])

        slot = lax.broadcasted_iota(jnp.int32, (CHUNK, 1), 0) + e * CHUNK
        is_mine = (slot >= mine_low) & (slot < mine_high)
        is_other = (slot >= other_low) & (slot < other_high)
        e_own = jnp.minimum(e, n_own - 1)
        zero = jnp.zeros((), jnp.float32)
        for cut in range(depth // CUT):
            cols = pl.ds(cut * CUT, CUT)
            first, second = older[:, cols], newer[:, cols]
            older[:, cols] = second
            forward = jnp.dot(shift[...], jnp.concatenate([first, second], axis=0), preferred_element_type=jnp.float32)
            from_mine = jnp.where(is_mine, mine[rows(e_own), cols].astype(jnp.float32), zero)
            from_other = jnp.where(is_other, other[rows(e_own), cols].astype(jnp.float32), zero)
            merged[rows(e), cols] = (from_mine + from_other + forward).astype(jnp.bfloat16)

        @pl.when(e < n_wire)
        def _():
            ring_copy(e).start()

        pair_copy(e).start()

        for cut in range(depth // CUT):
            cols = pl.ds(cut * CUT, CUT)

            def pick(c, acc):
                return jnp.where(c == e + 2 - delay, land[rows(c), cols], acc)

            newer[:, cols] = lax.fori_loop(jnp.maximum(e + 2 - max_delay, 0), e - LAG + 1, pick,
                                           jnp.zeros((CHUNK, CUT), land.dtype))

        @pl.when(e == 0)
        def _():
            out_ref[...] = jnp.zeros_like(out_ref)

        @pl.when(e >= 2)
        def _():
            p = e // 2 - 1
            piece = lax.rem(e, 2)

            @pl.when(e == 2)
            def _():
                hid_copy.wait()

            @pl.when(piece == 0)
            def _():
                pair_copy(2 * p).wait_recv()
                pair_copy(2 * p + 1).wait_recv()

            score(p, pl.multiple_of(piece * (n_rows // PIECES), n_rows // PIECES), n_rows // PIECES)

        return carry

    lax.fori_loop(0, n_all, step, 0)

    last = n_all // 2 - 1
    move(core, against(0, n_rows, merged[pair_rows(last), :]), last, 0, n_rows)
    pair_copy(2 * last).wait_recv()
    pair_copy(2 * last + 1).wait_recv()
    move(1 - core, against(0, n_rows, theirs[pair_rows(last), :]), last, 0, n_rows)

    def finish(e, c):
        @pl.when(e < n_own)
        def _():
            other_copy(e).wait_send()

        @pl.when(e < n_wire)
        def _():
            ring_copy(e).wait_send()

        pair_copy(e).wait_send()
        return c

    lax.fori_loop(0, n_all, finish, 0)


def softmax_kernel(s_ref, valid_ref, target_ref, probs_ref, logp_ref):
    s = s_ref[...]
    n = s.shape[0]
    eye = lax.broadcasted_iota(jnp.int32, (n, n), 0) == lax.broadcasted_iota(jnp.int32, (n, n), 1)
    target = jnp.sum(jnp.where(eye, target_ref[0], 0), axis=1, keepdims=True)
    masked = jnp.where(valid_ref[...] > 0, s, -jnp.inf)
    top = jnp.max(masked, axis=1, keepdims=True)
    power = jnp.exp(masked - top)
    total = jnp.sum(power, axis=1, keepdims=True)
    probs_ref[...] = power * (1.0 / total)
    lane = lax.broadcasted_iota(jnp.int32, s.shape, 1)
    picked = jnp.sum(jnp.where(lane == target, s, 0.0), axis=1, keepdims=True)
    logp = picked - (jnp.log(total) + top)
    logp_ref[0] = jnp.sum(jnp.where(eye, logp, 0.0), axis=0, keepdims=True)


def solution(mesh):
    shards = mesh.shape['vocab']

    def device_step(hidden, w_head, allowed_ids, allowed_valid, target_pos):
        list_len = allowed_ids.shape[0]
        half = list_len // 2
        vocab_local, depth = w_head.shape
        rows_dev = hidden.shape[0]
        chips = shards // 2
        ids = allowed_ids.reshape(2, half)
        rank = jnp.sum((ids[:, :, None] < ids[:, None, :]).astype(jnp.int32), axis=1)
        at = lax.broadcasted_iota(jnp.int32, (2, half, half), 1)
        sorted_ids = jnp.sum(jnp.where(rank[:, None, :] == at, ids[:, None, :], 0), axis=2)
        edges = lax.broadcasted_iota(jnp.int32, (2, shards + 1, half), 1) * vocab_local
        base = jnp.sum((ids[:, None, :] < edges).astype(jnp.int32), axis=2)

        gbuf = pl.pallas_call(
            gather_kernel,
            out_shape=jax.ShapeDtypeStruct((2, half, depth), w_head.dtype),
            in_specs=[pl.BlockSpec(memory_space=pltpu.SMEM), pl.BlockSpec(memory_space=pltpu.SMEM), pl.BlockSpec(memory_space=pl.ANY)],
            out_specs=pl.BlockSpec(memory_space=pl.ANY),
            scratch_shapes=[
                pltpu.VMEM((2, GATHER * PACK, depth), w_head.dtype),
                pltpu.VMEM((2, GATHER, GATHER * PACK), jnp.float32),
                pltpu.VMEM((2, GATHER, depth), w_head.dtype),
                pltpu.SemaphoreType.DMA((2,)),
                pltpu.SemaphoreType.DMA((2,)),
            ],
            name='gather_rows',
        )(base, sorted_ids, w_head)

        n_own = half // CHUNK
        n_wire = n_own + (chips - 2) * LAG
        n_all = n_own + (chips - 1) * LAG
        scores = pl.pallas_call(
            functools.partial(ring_kernel, shards),
            out_shape=jax.ShapeDtypeStruct((rows_dev, list_len), jnp.float32),
            in_specs=[pl.BlockSpec(memory_space=pltpu.SMEM), pl.BlockSpec(memory_space=pltpu.VMEM),
                      pl.BlockSpec(memory_space=pl.ANY), pl.BlockSpec(memory_space=pl.ANY)],
            out_specs=pl.BlockSpec(memory_space=pltpu.VMEM),
            scratch_shapes=[
                pltpu.VMEM((rows_dev, depth), hidden.dtype),
                pltpu.VMEM((half, depth), w_head.dtype),
                pltpu.VMEM((half, depth), w_head.dtype),
                pltpu.VMEM((n_wire * CHUNK, depth), w_head.dtype),
                pltpu.VMEM((n_all * CHUNK, depth), w_head.dtype),
                pltpu.VMEM((n_all * CHUNK, depth), w_head.dtype),
                pltpu.VMEM((2, 1, half), jnp.int32),
                pltpu.VMEM((CHUNK, 2 * CHUNK), jnp.bfloat16),
                pltpu.VMEM((CHUNK, depth), w_head.dtype),
                pltpu.VMEM((CHUNK, depth), w_head.dtype),
                pltpu.SemaphoreType.DMA,
                pltpu.SemaphoreType.DMA((n_own,)),
                pltpu.SemaphoreType.DMA((n_own,)),
                pltpu.SemaphoreType.DMA((n_own,)),
                pltpu.SemaphoreType.DMA((n_wire,)),
                pltpu.SemaphoreType.DMA((n_wire,)),
                pltpu.SemaphoreType.DMA((n_all,)),
                pltpu.SemaphoreType.DMA((n_all,)),
            ],
            compiler_params=pltpu.CompilerParams(collective_id=0, has_side_effects=True, vmem_limit_bytes=62 * 1024 * 1024),
            name='ring_scores',
        )(base, rank, hidden, gbuf)

        tile = 128
        probs, logp = pl.pallas_call(
            softmax_kernel,
            grid=(rows_dev // tile,),
            out_shape=[jax.ShapeDtypeStruct((rows_dev, list_len), jnp.float32), jax.ShapeDtypeStruct((rows_dev // tile, 1, tile), jnp.float32)],
            in_specs=[pl.BlockSpec((tile, list_len), lambda i: (i, 0)), pl.BlockSpec((1, list_len), lambda i: (0, 0)),
                      pl.BlockSpec((1, 1, tile), lambda i: (i, 0, 0))],
            out_specs=[pl.BlockSpec((tile, list_len), lambda i: (i, 0)), pl.BlockSpec((1, 1, tile), lambda i: (i, 0, 0))],
            name='softmax',
        )(scores, allowed_valid.reshape(1, list_len), target_pos.reshape(rows_dev // tile, 1, tile))
        return probs, logp.reshape(rows_dev)

    row_spec = P(('rep', 'vocab'))
    mat_spec = P(('rep', 'vocab'), None)
    return jax.shard_map(device_step, mesh=mesh, in_specs=(mat_spec, P('vocab', None), P('rep'), P('rep'), row_spec), out_specs=(mat_spec, row_spec), check_vma=False)
```

```python
import functools

import jax
import jax.numpy as jnp
from jax import lax
from jax.experimental import pallas as pl
from jax.experimental.pallas import tpu as pltpu
from jax.sharding import PartitionSpec as P

INV_TEMP = 1.25
MESH = pl.DeviceIdType.MESH
CHUNK = 64
LAG = 2
GATHER = 32
PACK_BITS = 1
PACK = 1 << PACK_BITS
SCORED = 128
PIECES = 2
STAGES = 4
CUT = 768


def gather_kernel(shards, base_ref, sid_ref, w_ref, gbuf_ref, stage, pick, in_sem):
    v = lax.axis_index('vocab')
    vocab_local = w_ref.shape[0]
    half = gbuf_ref.shape[1]
    chip = v // 2

    def span(k):
        at = k * (shards + 1)
        first = base_ref[at + v]
        count = base_ref[at + v + 1] - first
        slot0 = first - base_ref[at + 2 * chip]
        block0 = slot0 // GATHER
        blocks = jnp.where(count > 0, (slot0 + count + GATHER - 1) // GATHER - block0, 0)
        return first, count, slot0, block0, blocks

    spans = [span(0), span(1)]
    total = spans[0][4] + spans[1][4]

    def where_is(t):
        second = t >= spans[0][4]
        first, count, slot0, block0 = [jnp.where(second, spans[1][i], spans[0][i]) for i in range(4)]
        k = jnp.where(second, 1, 0)
        block = block0 + jnp.where(second, t - spans[0][4], t)
        lo = jnp.maximum(slot0 - block * GATHER, 0)
        last = jnp.minimum(slot0 + count - block * GATHER, GATHER) - 1
        src = first + block * GATHER - slot0
        return k, block, lo, last, src

    def row_copy(group, s, b):
        return pltpu.make_async_copy(
            w_ref.at[pl.ds(pl.multiple_of(group * PACK, PACK), PACK), :],
            stage.at[b, s],
            in_sem.at[b])

    lane = lax.broadcasted_iota(jnp.int32, (1, GATHER * PACK), 1)

    def issue(t, b):
        k, first, last, src = where_is(t)[0], *where_is(t)[2:]
        for s in range(GATHER):
            local = sid_ref[k, src + jnp.clip(s, first, last)] - v * vocab_local
            group = lax.shift_right_logical(local, PACK_BITS)
            row_copy(group, s, b).start()
            pick[b, pl.ds(s, 1), :] = jnp.where(lane == s * PACK + (local & (PACK - 1)), 1.0, 0.0)

    def begin(t, carry):
        issue(t, t)
        return carry

    def wait_stage(b):
        pltpu.make_async_copy(stage.at[b], stage.at[b], in_sem.at[b]).wait()

    def step(t, carry):
        b = lax.rem(t, STAGES)

        @pl.when(t + STAGES - 1 < total)
        def _():
            issue(t + STAGES - 1, lax.rem(t + STAGES - 1, STAGES))

        wait_stage(b)
        k, block = where_is(t)[:2]
        gbuf_ref[k, pl.ds(pl.multiple_of(block * GATHER, GATHER), GATHER), :] = jnp.dot(
            pick[b].astype(jnp.bfloat16), stage[b].reshape(GATHER * PACK, stage.shape[3]),
            preferred_element_type=jnp.float32).astype(gbuf_ref.dtype)
        return carry

    lax.fori_loop(0, jnp.minimum(total, STAGES - 1), begin, 0)
    lax.fori_loop(0, total, step, 0)


def ring_kernel(shards, base_ref, rank_ref, hid, gbuf_ref, out_ref,
                other, land, merged, theirs, slot_of, shift, older, newer,
                other_send, other_recv, ring_send, ring_recv, pair_send, pair_recv):
    chips = shards // 2
    half = gbuf_ref.shape[1]
    lag_rows = LAG * CHUNK
    n_own = half // CHUNK
    n_wire = n_own + (chips - 2) * LAG
    n_all = n_own + (chips - 1) * LAG
    max_delay = half // CHUNK + 1
    group = SCORED // CHUNK
    pad = -n_all % group
    gap = group // PIECES
    depth = hid.shape[1]
    v = lax.axis_index('vocab')
    core = lax.rem(v, 2)
    chip = v // 2
    partner = chip * 2 + 1 - core
    ahead = lax.rem(chip + 2 * core - 1 + chips, chips) * 2 + core
    behind = lax.rem(chip - 2 * core + 1 + chips, chips) * 2 + core

    barrier = pltpu.get_barrier_semaphore()
    for peer in (partner, ahead, behind):
        pl.semaphore_signal(barrier, inc=1, device_id={'vocab': peer}, device_id_type=MESH)

    def rows(e, n=CHUNK):
        return pl.ds(pl.multiple_of(e * CHUNK, CHUNK), n)

    def other_copy(e):
        return pltpu.make_async_remote_copy(
            src_ref=gbuf_ref.at[1 - core, rows(e), :], dst_ref=other.at[rows(e), :],
            send_sem=other_send.at[e], recv_sem=other_recv.at[e], device_id={'vocab': partner}, device_id_type=MESH)

    def ring_copy(e):
        return pltpu.make_async_remote_copy(
            src_ref=merged.at[rows(e + pad), :], dst_ref=land.at[rows(e), :],
            send_sem=ring_send.at[e], recv_sem=ring_recv.at[e], device_id={'vocab': ahead}, device_id_type=MESH)

    def pair_copy(e):
        return pltpu.make_async_remote_copy(
            src_ref=merged.at[rows(e + pad), :], dst_ref=theirs.at[rows(e + pad), :],
            send_sem=pair_send.at[e], recv_sem=pair_recv.at[e], device_id={'vocab': partner}, device_id_type=MESH)

    def base(k, w):
        return base_ref[k * (shards + 1) + w]

    pl.semaphore_wait(barrier, 3)
    ahead_of_use = 3
    for e in range(ahead_of_use):
        other_copy(e).start()

    for k in range(2):
        rank = rank_ref[pl.ds(k, 1), :]
        slots = jnp.zeros_like(rank)
        passed = jnp.int32(0)
        for hop in range(chips):
            owner = lax.rem(chip - (2 * k - 1) * hop + chips, chips)
            low, high = base(k, 2 * owner), base(k, 2 * owner + 2)
            slots += jnp.where((rank >= low) & (rank < high), rank + (passed - low), 0)
            passed += jnp.maximum(high - low, lag_rows)
        slot_of[k] = slots + pad * CHUNK
    if pad:
        merged[pl.ds(0, pad * CHUNK), :] = jnp.zeros((pad * CHUNK, depth), merged.dtype)
        theirs[pl.ds(0, pad * CHUNK), :] = jnp.zeros((pad * CHUNK, depth), theirs.dtype)
    older[...] = jnp.zeros_like(older)
    newer[...] = jnp.zeros_like(newer)

    chip_low = base(core, 2 * chip)
    own_pad = jnp.maximum(base(core, 2 * chip + 2) - chip_low, lag_rows)
    delay = (own_pad + CHUNK - 1) // CHUNK
    row = lax.broadcasted_iota(jnp.int32, (CHUNK, 2 * CHUNK), 0)
    col = lax.broadcasted_iota(jnp.int32, (CHUNK, 2 * CHUNK), 1)
    shift[...] = jnp.where(col == row + delay * CHUNK - own_pad, 1.0, 0.0).astype(jnp.bfloat16)
    mine_low = base(core, v) - chip_low
    mine_high = base(core, v + 1) - chip_low
    other_low = base(core, partner) - chip_low
    other_high = base(core, partner + 1) - chip_low

    def move(k, s, p, at, n):
        top = s.astype(jnp.bfloat16)
        rest = s - top.astype(jnp.float32)
        mid = rest.astype(jnp.bfloat16)
        low = (rest - mid.astype(jnp.float32)).astype(jnp.bfloat16)
        slot = lax.broadcasted_iota(jnp.int32, (SCORED, half), 0) + p * SCORED
        place = jnp.where(slot == slot_of[k], 1.0, 0.0).astype(jnp.bfloat16)
        moved = jnp.dot(jnp.concatenate([top, mid, low], axis=1), jnp.concatenate([place] * 3, axis=0),
                        preferred_element_type=jnp.float32)
        spot = (pl.ds(at, n), pl.ds(pl.multiple_of(k * half, half), half))
        out_ref[spot] = out_ref[spot] + moved

    def group_rows(p):
        return pl.ds(pl.multiple_of(p * SCORED, SCORED), SCORED)

    def against(at, n, part):
        return lax.dot_general(hid[pl.ds(at, n), :], part, (((1,), (1,)), ((), ())), preferred_element_type=jnp.float32) * INV_TEMP

    n_rows = hid.shape[0]

    def score(p, at, n):
        s = against(at, n, jnp.concatenate([merged[group_rows(p), :], theirs[group_rows(p), :]], axis=0))
        move(core, s[:, :SCORED], p, at, n)
        move(1 - core, s[:, SCORED:], p, at, n)

    def wait_theirs(p):
        for j in range(group):
            at = p * group + j - pad

            @pl.when(at >= 0)
            def _():
                pair_copy(at).wait_recv()

    def step(e, carry):
        @pl.when(e + ahead_of_use < n_own)
        def _():
            other_copy(e + ahead_of_use).start()

        @pl.when(e < n_own)
        def _():
            other_copy(e).wait_recv()

        @pl.when(e >= LAG)
        def _():
            ring_copy(e - LAG).wait_recv()
            for cut in range(depth // CUT):
                cols = pl.ds(cut * CUT, CUT)
                fresh = land[rows(e - LAG), cols]
                older[:, cols] = jnp.where(delay == LAG, fresh, older[:, cols])
                newer[:, cols] = jnp.where(delay == LAG + 1, fresh, newer[:, cols])

        slot = lax.broadcasted_iota(jnp.int32, (CHUNK, 1), 0) + e * CHUNK
        is_mine = (slot >= mine_low) & (slot < mine_high)
        is_other = (slot >= other_low) & (slot < other_high)
        e_own = jnp.minimum(e, n_own - 1)
        zero = jnp.zeros((), jnp.float32)
        for cut in range(depth // CUT):
            cols = pl.ds(cut * CUT, CUT)
            first, second = older[:, cols], newer[:, cols]
            older[:, cols] = second
            forward = jnp.dot(shift[...], jnp.concatenate([first, second], axis=0), preferred_element_type=jnp.float32)
            from_mine = jnp.where(is_mine, gbuf_ref[core, rows(e_own), cols].astype(jnp.float32), zero)
            from_other = jnp.where(is_other, other[rows(e_own), cols].astype(jnp.float32), zero)
            merged[rows(e + pad), cols] = (from_mine + from_other + forward).astype(jnp.bfloat16)

        @pl.when(e < n_wire)
        def _():
            ring_copy(e).start()

        pair_copy(e).start()

        for cut in range(depth // CUT):
            cols = pl.ds(cut * CUT, CUT)

            def pick(c, acc):
                return jnp.where(c == e + 2 - delay, land[rows(c), cols], acc)

            newer[:, cols] = lax.fori_loop(jnp.maximum(e + 2 - max_delay, 0), e - LAG + 1, pick,
                                           jnp.zeros((CHUNK, CUT), land.dtype))

        @pl.when(e == 0)
        def _():
            out_ref[...] = jnp.zeros_like(out_ref)

        since = e - (group - 1 - pad)

        @pl.when((since >= gap) & (lax.rem(since, gap) == 0) & (e < n_all - 1))
        def _():
            p = (since // gap - 1) // PIECES
            piece = lax.rem(since // gap - 1, PIECES)

            @pl.when(piece == 0)
            def _():
                wait_theirs(p)

            def one(i, c):
                score(p, pl.multiple_of(i * (n_rows // PIECES), n_rows // PIECES), n_rows // PIECES)
                return c

            lax.fori_loop(piece, jnp.where(e == n_all - 2, PIECES, piece + 1), one, 0)

        return carry

    lax.fori_loop(0, n_all, step, 0)

    last = (n_all + pad) // group - 1
    move(core, against(0, n_rows, merged[group_rows(last), :]), last, 0, n_rows)
    wait_theirs(last)
    move(1 - core, against(0, n_rows, theirs[group_rows(last), :]), last, 0, n_rows)

    def finish(e, c):
        @pl.when(e < n_own)
        def _():
            other_copy(e).wait_send()

        @pl.when(e < n_wire)
        def _():
            ring_copy(e).wait_send()

        pair_copy(e).wait_send()
        return c

    lax.fori_loop(0, n_all, finish, 0)


def softmax_kernel(s_ref, valid_ref, target_ref, probs_ref, logp_ref):
    n = probs_ref.shape[0]
    s = s_ref[pl.ds(pl.multiple_of(pl.program_id(0) * n, n), n), :]
    eye = lax.broadcasted_iota(jnp.int32, (n, n), 0) == lax.broadcasted_iota(jnp.int32, (n, n), 1)
    target = jnp.sum(jnp.where(eye, target_ref[0], 0), axis=1, keepdims=True)
    masked = jnp.where(valid_ref[...] > 0, s, -jnp.inf)
    top = jnp.max(masked, axis=1, keepdims=True)
    power = jnp.exp(masked - top)
    total = jnp.sum(power, axis=1, keepdims=True)
    probs_ref[...] = power * (1.0 / total)
    lane = lax.broadcasted_iota(jnp.int32, s.shape, 1)
    picked = jnp.sum(jnp.where(lane == target, s, 0.0), axis=1, keepdims=True)
    logp = picked - (jnp.log(total) + top)
    logp_ref[0] = jnp.sum(jnp.where(eye, logp, 0.0), axis=0, keepdims=True)


def solution(mesh):
    shards = mesh.shape['vocab']

    def device_step(hidden, w_head, allowed_ids, allowed_valid, target_pos):
        list_len = allowed_ids.shape[0]
        half = list_len // 2
        vocab_local, depth = w_head.shape
        rows_dev = hidden.shape[0]
        chips = shards // 2
        ids = allowed_ids.reshape(2, half)
        rank = jnp.sum((ids[:, :, None] < ids[:, None, :]).astype(jnp.int32), axis=1)
        at = lax.broadcasted_iota(jnp.int32, (2, half, half), 1)
        sorted_ids = jnp.sum(jnp.where(rank[:, None, :] == at, ids[:, None, :], 0), axis=2)
        edges = lax.broadcasted_iota(jnp.int32, (2, shards + 1, half), 1) * vocab_local
        base = jnp.sum((ids[:, None, :] < edges).astype(jnp.int32).reshape(2 * (shards + 1), half), axis=1)

        gbuf = pl.pallas_call(
            functools.partial(gather_kernel, shards),
            out_shape=jax.ShapeDtypeStruct((2, half, depth), w_head.dtype),
            in_specs=[pl.BlockSpec(memory_space=pltpu.SMEM), pl.BlockSpec(memory_space=pltpu.SMEM), pl.BlockSpec(memory_space=pl.ANY)],
            out_specs=pl.BlockSpec(memory_space=pltpu.VMEM),
            scratch_shapes=[
                pltpu.VMEM((STAGES, GATHER, PACK, depth), w_head.dtype),
                pltpu.VMEM((STAGES, GATHER, GATHER * PACK), jnp.float32),
                pltpu.SemaphoreType.DMA((STAGES,)),
            ],
            compiler_params=pltpu.CompilerParams(vmem_limit_bytes=20 * 1024 * 1024),
            name='gather_rows',
        )(base, sorted_ids, w_head)

        n_own = half // CHUNK
        n_wire = n_own + (chips - 2) * LAG
        n_all = n_own + (chips - 1) * LAG
        scores = pl.pallas_call(
            functools.partial(ring_kernel, shards),
            out_shape=jax.ShapeDtypeStruct((rows_dev, list_len), jnp.float32),
            in_specs=[pl.BlockSpec(memory_space=pltpu.SMEM), pl.BlockSpec(memory_space=pltpu.VMEM),
                      pl.BlockSpec(memory_space=pltpu.VMEM), pl.BlockSpec(memory_space=pltpu.VMEM)],
            out_specs=pl.BlockSpec(memory_space=pltpu.VMEM),
            scratch_shapes=[
                pltpu.VMEM((half, depth), w_head.dtype),
                pltpu.VMEM((n_wire * CHUNK, depth), w_head.dtype),
                pltpu.VMEM((pl.cdiv(n_all * CHUNK, SCORED) * SCORED, depth), w_head.dtype),
                pltpu.VMEM((pl.cdiv(n_all * CHUNK, SCORED) * SCORED, depth), w_head.dtype),
                pltpu.VMEM((2, 1, half), jnp.int32),
                pltpu.VMEM((CHUNK, 2 * CHUNK), jnp.bfloat16),
                pltpu.VMEM((CHUNK, depth), w_head.dtype),
                pltpu.VMEM((CHUNK, depth), w_head.dtype),
                pltpu.SemaphoreType.DMA((n_own,)),
                pltpu.SemaphoreType.DMA((n_own,)),
                pltpu.SemaphoreType.DMA((n_wire,)),
                pltpu.SemaphoreType.DMA((n_wire,)),
                pltpu.SemaphoreType.DMA((n_all,)),
                pltpu.SemaphoreType.DMA((n_all,)),
            ],
            compiler_params=pltpu.CompilerParams(collective_id=0, has_side_effects=True, vmem_limit_bytes=34 * 1024 * 1024),
            name='ring_scores',
        )(base, rank, hidden, gbuf)

        tile = 128
        probs, logp = pl.pallas_call(
            softmax_kernel,
            grid=(rows_dev // tile,),
            out_shape=[jax.ShapeDtypeStruct((rows_dev, list_len), jnp.float32), jax.ShapeDtypeStruct((rows_dev // tile, 1, tile), jnp.float32)],
            in_specs=[pl.BlockSpec(memory_space=pltpu.VMEM), pl.BlockSpec((1, list_len), lambda i: (0, 0)),
                      pl.BlockSpec((1, 1, tile), lambda i: (i, 0, 0))],
            out_specs=[pl.BlockSpec((tile, list_len), lambda i: (i, 0)), pl.BlockSpec((1, 1, tile), lambda i: (i, 0, 0))],
            compiler_params=pltpu.CompilerParams(vmem_limit_bytes=24 * 1024 * 1024),
            name='softmax',
        )(scores, allowed_valid.reshape(1, list_len), target_pos.reshape(rows_dev // tile, 1, tile))
        return probs, logp.reshape(rows_dev)

    row_spec = P(('rep', 'vocab'))
    mat_spec = P(('rep', 'vocab'), None)
    return jax.shard_map(device_step, mesh=mesh, in_specs=(mat_spec, P('vocab', None), P('rep'), P('rep'), row_spec), out_specs=(mat_spec, row_spec), check_vma=False)
```

```python
import functools

import jax
import jax.numpy as jnp
from jax import lax
from jax.experimental import pallas as pl
from jax.experimental.pallas import tpu as pltpu
from jax.sharding import PartitionSpec as P

INV_TEMP = 1.25
MESH = pl.DeviceIdType.MESH
CHUNK = 64
LAG = 2
GATHER = 32
PACK_BITS = 1
PACK = 1 << PACK_BITS
SCORED = 128
PIECES = 2
STAGES = 4
CUT = 768


def gather_kernel(shards, base_ref, local_ref, w_ref, gbuf_ref, stage, pick, in_sem):
    v = lax.axis_index('vocab')
    chip = v // 2

    def span(k):
        at = k * (shards + 1)
        first = base_ref[at + v]
        count = base_ref[at + v + 1] - first
        slot0 = first - base_ref[at + 2 * chip]
        block0 = slot0 // GATHER
        blocks = jnp.where(count > 0, (slot0 + count + GATHER - 1) // GATHER - block0, 0)
        return first, slot0, block0, blocks

    spans = [span(0), span(1)]
    total = spans[0][3] + spans[1][3]

    def where_is(t):
        second = t >= spans[0][3]
        first, slot0, block0 = [jnp.where(second, spans[1][i], spans[0][i]) for i in range(3)]
        k = jnp.where(second, 1, 0)
        block = block0 + jnp.where(second, t - spans[0][3], t)
        return k, block, first - slot0 + block * GATHER

    def row_copy(group, s, b):
        return pltpu.make_async_copy(
            w_ref.at[pl.ds(pl.multiple_of(group * PACK, PACK), PACK), :],
            stage.at[b, s],
            in_sem.at[b])

    lane = lax.broadcasted_iota(jnp.int32, (1, GATHER * PACK), 1)

    def issue(t, b):
        k, _, src = where_is(t)
        for s in range(GATHER):
            local = local_ref[k, src + s]
            group = lax.shift_right_logical(local, PACK_BITS)
            row_copy(group, s, b).start()
            pick[b, pl.ds(s, 1), :] = jnp.where(lane == s * PACK + (local & (PACK - 1)), 1.0, 0.0)

    def begin(t, carry):
        issue(t, t)
        return carry

    def wait_stage(b):
        pltpu.make_async_copy(stage.at[b], stage.at[b], in_sem.at[b]).wait()

    def step(t, carry):
        b = lax.rem(t, STAGES)

        @pl.when(t + STAGES - 1 < total)
        def _():
            issue(t + STAGES - 1, lax.rem(t + STAGES - 1, STAGES))

        wait_stage(b)
        k, block, _ = where_is(t)
        gbuf_ref[k, pl.ds(pl.multiple_of(block * GATHER, GATHER), GATHER), :] = jnp.dot(
            pick[b].astype(jnp.bfloat16), stage[b].reshape(GATHER * PACK, stage.shape[3]),
            preferred_element_type=jnp.float32).astype(gbuf_ref.dtype)
        return carry

    lax.fori_loop(0, jnp.minimum(total, STAGES - 1), begin, 0)
    lax.fori_loop(0, total, step, 0)


def ring_kernel(shards, base_ref, rank_ref, hid, gbuf_ref, out_ref,
                other, land, merged, theirs, slot_of, shift, older, newer,
                other_send, other_recv, ring_send, ring_recv, pair_send, pair_recv):
    chips = shards // 2
    half = gbuf_ref.shape[1]
    lag_rows = LAG * CHUNK
    n_own = half // CHUNK
    n_wire = n_own + (chips - 2) * LAG
    n_all = n_own + (chips - 1) * LAG
    max_delay = half // CHUNK + 1
    group = SCORED // CHUNK
    pad = -n_all % group
    gap = group // PIECES
    final = n_all - 1 - group + gap
    depth = hid.shape[1]
    v = lax.axis_index('vocab')
    core = lax.rem(v, 2)
    chip = v // 2
    partner = chip * 2 + 1 - core
    ahead = lax.rem(chip + 2 * core - 1 + chips, chips) * 2 + core
    behind = lax.rem(chip - 2 * core + 1 + chips, chips) * 2 + core

    barrier = pltpu.get_barrier_semaphore()
    for peer in (partner, ahead, behind):
        pl.semaphore_signal(barrier, inc=1, device_id={'vocab': peer}, device_id_type=MESH)

    def rows(e, n=CHUNK):
        return pl.ds(pl.multiple_of(e * CHUNK, CHUNK), n)

    def other_copy(e):
        return pltpu.make_async_remote_copy(
            src_ref=gbuf_ref.at[1 - core, rows(e), :], dst_ref=other.at[rows(e), :],
            send_sem=other_send.at[e], recv_sem=other_recv.at[e], device_id={'vocab': partner}, device_id_type=MESH)

    def ring_copy(e):
        return pltpu.make_async_remote_copy(
            src_ref=merged.at[rows(e + pad), :], dst_ref=land.at[rows(e), :],
            send_sem=ring_send.at[e], recv_sem=ring_recv.at[e], device_id={'vocab': ahead}, device_id_type=MESH)

    def pair_copy(e):
        return pltpu.make_async_remote_copy(
            src_ref=merged.at[rows(e + pad), :], dst_ref=theirs.at[rows(e + pad), :],
            send_sem=pair_send.at[e], recv_sem=pair_recv.at[e], device_id={'vocab': partner}, device_id_type=MESH)

    def base(k, w):
        return base_ref[k * (shards + 1) + w]

    pl.semaphore_wait(barrier, 3)
    ahead_of_use = 3
    for e in range(ahead_of_use):
        other_copy(e).start()

    for k in range(2):
        rank = rank_ref[pl.ds(k, 1), :]
        slots = jnp.zeros_like(rank)
        passed = jnp.int32(0)
        for hop in range(chips):
            owner = lax.rem(chip - (2 * k - 1) * hop + chips, chips)
            low, high = base(k, 2 * owner), base(k, 2 * owner + 2)
            slots += jnp.where((rank >= low) & (rank < high), rank + (passed - low), 0)
            passed += jnp.maximum(high - low, lag_rows)
        slot_of[k] = slots + pad * CHUNK
    if pad:
        merged[pl.ds(0, pad * CHUNK), :] = jnp.zeros((pad * CHUNK, depth), merged.dtype)
        theirs[pl.ds(0, pad * CHUNK), :] = jnp.zeros((pad * CHUNK, depth), theirs.dtype)
    older[...] = jnp.zeros_like(older)
    newer[...] = jnp.zeros_like(newer)

    chip_low = base(core, 2 * chip)
    own_pad = jnp.maximum(base(core, 2 * chip + 2) - chip_low, lag_rows)
    delay = (own_pad + CHUNK - 1) // CHUNK
    row = lax.broadcasted_iota(jnp.int32, (CHUNK, 2 * CHUNK), 0)
    col = lax.broadcasted_iota(jnp.int32, (CHUNK, 2 * CHUNK), 1)
    shift[...] = jnp.where(col == row + delay * CHUNK - own_pad, 1.0, 0.0).astype(jnp.bfloat16)
    mine_low = base(core, v) - chip_low
    mine_high = base(core, v + 1) - chip_low
    other_low = base(core, partner) - chip_low
    other_high = base(core, partner + 1) - chip_low

    def move(k, s, p, at, n):
        top = s.astype(jnp.bfloat16)
        rest = s - top.astype(jnp.float32)
        mid = rest.astype(jnp.bfloat16)
        low = (rest - mid.astype(jnp.float32)).astype(jnp.bfloat16)
        slot = lax.broadcasted_iota(jnp.int32, (SCORED, half), 0) + p * SCORED
        place = jnp.where(slot == slot_of[k], 1.0, 0.0).astype(jnp.bfloat16)
        moved = jnp.dot(jnp.concatenate([top, mid, low], axis=1), jnp.concatenate([place] * 3, axis=0),
                        preferred_element_type=jnp.float32)
        spot = (pl.ds(at, n), pl.ds(pl.multiple_of(k * half, half), half))
        out_ref[spot] = out_ref[spot] + moved

    def group_rows(p):
        return pl.ds(pl.multiple_of(p * SCORED, SCORED), SCORED)

    def against(at, n, part):
        return lax.dot_general(hid[pl.ds(at, n), :], part, (((1,), (1,)), ((), ())), preferred_element_type=jnp.float32) * INV_TEMP

    n_rows = hid.shape[0]

    def score(p, at, n):
        s = against(at, n, jnp.concatenate([merged[group_rows(p), :], theirs[group_rows(p), :]], axis=0))
        move(core, s[:, :SCORED], p, at, n)
        move(1 - core, s[:, SCORED:], p, at, n)

    def wait_theirs(p):
        for j in range(group):
            at = p * group + j - pad

            @pl.when(at >= 0)
            def _():
                pair_copy(at).wait_recv()

    def step(e, carry):
        @pl.when(e + ahead_of_use < n_own)
        def _():
            other_copy(e + ahead_of_use).start()

        @pl.when(e < n_own)
        def _():
            other_copy(e).wait_recv()

        @pl.when(e >= LAG)
        def _():
            ring_copy(e - LAG).wait_recv()
            for cut in range(depth // CUT):
                cols = pl.ds(cut * CUT, CUT)
                fresh = land[rows(e - LAG), cols]
                older[:, cols] = jnp.where(delay == LAG, fresh, older[:, cols])
                newer[:, cols] = jnp.where(delay == LAG + 1, fresh, newer[:, cols])

        slot = lax.broadcasted_iota(jnp.int32, (CHUNK, 1), 0) + e * CHUNK
        is_mine = (slot >= mine_low) & (slot < mine_high)
        is_other = (slot >= other_low) & (slot < other_high)
        e_own = jnp.minimum(e, n_own - 1)
        zero = jnp.zeros((), jnp.float32)
        for cut in range(depth // CUT):
            cols = pl.ds(cut * CUT, CUT)
            first, second = older[:, cols], newer[:, cols]
            older[:, cols] = second
            forward = jnp.dot(shift[...], jnp.concatenate([first, second], axis=0), preferred_element_type=jnp.float32)
            from_mine = jnp.where(is_mine, gbuf_ref[core, rows(e_own), cols].astype(jnp.float32), zero)
            from_other = jnp.where(is_other, other[rows(e_own), cols].astype(jnp.float32), zero)
            merged[rows(e + pad), cols] = (from_mine + from_other + forward).astype(jnp.bfloat16)

        @pl.when(e < n_wire)
        def _():
            ring_copy(e).start()

        pair_copy(e).start()

        for cut in range(depth // CUT):
            cols = pl.ds(cut * CUT, CUT)

            def pick(c, acc):
                return jnp.where(c == e + 2 - delay, land[rows(c), cols], acc)

            newer[:, cols] = lax.fori_loop(jnp.maximum(e + 2 - max_delay, 0), e - LAG + 1, pick,
                                           jnp.zeros((CHUNK, CUT), land.dtype))

        @pl.when(e == 0)
        def _():
            out_ref[...] = jnp.zeros_like(out_ref)

        since = e - (group - 1 - pad)

        @pl.when((since >= gap) & (lax.rem(since, gap) == 0) & (e <= final))
        def _():
            p = (since // gap - 1) // PIECES
            piece = lax.rem(since // gap - 1, PIECES)

            @pl.when(piece == 0)
            def _():
                wait_theirs(p)

            def one(i, c):
                score(p, pl.multiple_of(i * (n_rows // PIECES), n_rows // PIECES), n_rows // PIECES)
                return c

            lax.fori_loop(piece, jnp.where(e == final, PIECES, piece + 1), one, 0)

        return carry

    lax.fori_loop(0, n_all, step, 0)

    last = (n_all + pad) // group - 1
    move(core, against(0, n_rows, merged[group_rows(last), :]), last, 0, n_rows)
    wait_theirs(last)
    move(1 - core, against(0, n_rows, theirs[group_rows(last), :]), last, 0, n_rows)

    def finish(e, c):
        @pl.when(e < n_own)
        def _():
            other_copy(e).wait_send()

        @pl.when(e < n_wire)
        def _():
            ring_copy(e).wait_send()

        pair_copy(e).wait_send()
        return c

    lax.fori_loop(0, n_all, finish, 0)


def softmax_kernel(s_ref, valid_ref, target_ref, probs_ref, logp_ref):
    n = probs_ref.shape[0]
    s = s_ref[pl.ds(pl.multiple_of(pl.program_id(0) * n, n), n), :]
    eye = lax.broadcasted_iota(jnp.int32, (n, n), 0) == lax.broadcasted_iota(jnp.int32, (n, n), 1)
    target = jnp.sum(jnp.where(eye, target_ref[0], 0), axis=1, keepdims=True)
    masked = jnp.where(valid_ref[...] > 0, s, -jnp.inf)
    top = jnp.max(masked, axis=1, keepdims=True)
    power = jnp.exp(masked - top)
    total = jnp.sum(power, axis=1, keepdims=True)
    probs_ref[...] = power * (1.0 / total)
    lane = lax.broadcasted_iota(jnp.int32, s.shape, 1)
    picked = jnp.sum(jnp.where(lane == target, s, 0.0), axis=1, keepdims=True)
    logp = picked - (jnp.log(total) + top)
    logp_ref[0] = jnp.sum(jnp.where(eye, logp, 0.0), axis=0, keepdims=True)


def solution(mesh):
    shards = mesh.shape['vocab']

    def device_step(hidden, w_head, allowed_ids, allowed_valid, target_pos):
        list_len = allowed_ids.shape[0]
        half = list_len // 2
        vocab_local, depth = w_head.shape
        rows_dev = hidden.shape[0]
        chips = shards // 2
        ids = allowed_ids.reshape(2, half)
        rank = jnp.sum((ids[:, :, None] < ids[:, None, :]).astype(jnp.int32), axis=1)
        at = lax.broadcasted_iota(jnp.int32, (2, half + GATHER, half), 1)
        sorted_ids = jnp.sum(jnp.where(rank[:, None, :] == at, ids[:, None, :], 0), axis=2)
        local = jnp.clip(sorted_ids - lax.axis_index('vocab') * vocab_local, 0, vocab_local - 1)
        edges = lax.broadcasted_iota(jnp.int32, (2, shards + 1, half), 1) * vocab_local
        base = jnp.sum((ids[:, None, :] < edges).astype(jnp.int32).reshape(2 * (shards + 1), half), axis=1)

        gbuf = pl.pallas_call(
            functools.partial(gather_kernel, shards),
            out_shape=jax.ShapeDtypeStruct((2, half, depth), w_head.dtype),
            in_specs=[pl.BlockSpec(memory_space=pltpu.SMEM), pl.BlockSpec(memory_space=pltpu.SMEM), pl.BlockSpec(memory_space=pl.ANY)],
            out_specs=pl.BlockSpec(memory_space=pltpu.VMEM),
            scratch_shapes=[
                pltpu.VMEM((STAGES, GATHER, PACK, depth), w_head.dtype),
                pltpu.VMEM((STAGES, GATHER, GATHER * PACK), jnp.float32),
                pltpu.SemaphoreType.DMA((STAGES,)),
            ],
            compiler_params=pltpu.CompilerParams(vmem_limit_bytes=20 * 1024 * 1024),
            name='gather_rows',
        )(base, local, w_head)

        n_own = half // CHUNK
        n_wire = n_own + (chips - 2) * LAG
        n_all = n_own + (chips - 1) * LAG
        scores = pl.pallas_call(
            functools.partial(ring_kernel, shards),
            out_shape=jax.ShapeDtypeStruct((rows_dev, list_len), jnp.float32),
            in_specs=[pl.BlockSpec(memory_space=pltpu.SMEM), pl.BlockSpec(memory_space=pltpu.VMEM),
                      pl.BlockSpec(memory_space=pltpu.VMEM), pl.BlockSpec(memory_space=pltpu.VMEM)],
            out_specs=pl.BlockSpec(memory_space=pltpu.VMEM),
            scratch_shapes=[
                pltpu.VMEM((half, depth), w_head.dtype),
                pltpu.VMEM((n_wire * CHUNK, depth), w_head.dtype),
                pltpu.VMEM((pl.cdiv(n_all * CHUNK, SCORED) * SCORED, depth), w_head.dtype),
                pltpu.VMEM((pl.cdiv(n_all * CHUNK, SCORED) * SCORED, depth), w_head.dtype),
                pltpu.VMEM((2, 1, half), jnp.int32),
                pltpu.VMEM((CHUNK, 2 * CHUNK), jnp.bfloat16),
                pltpu.VMEM((CHUNK, depth), w_head.dtype),
                pltpu.VMEM((CHUNK, depth), w_head.dtype),
                pltpu.SemaphoreType.DMA((n_own,)),
                pltpu.SemaphoreType.DMA((n_own,)),
                pltpu.SemaphoreType.DMA((n_wire,)),
                pltpu.SemaphoreType.DMA((n_wire,)),
                pltpu.SemaphoreType.DMA((n_all,)),
                pltpu.SemaphoreType.DMA((n_all,)),
            ],
            compiler_params=pltpu.CompilerParams(collective_id=0, has_side_effects=True, vmem_limit_bytes=34 * 1024 * 1024),
            name='ring_scores',
        )(base, rank, hidden, gbuf)

        tile = 256
        probs, logp = pl.pallas_call(
            softmax_kernel,
            grid=(rows_dev // tile,),
            out_shape=[jax.ShapeDtypeStruct((rows_dev, list_len), jnp.float32), jax.ShapeDtypeStruct((rows_dev // tile, 1, tile), jnp.float32)],
            in_specs=[pl.BlockSpec(memory_space=pltpu.VMEM), pl.BlockSpec((1, list_len), lambda i: (0, 0)),
                      pl.BlockSpec((1, 1, tile), lambda i: (i, 0, 0))],
            out_specs=[pl.BlockSpec((tile, list_len), lambda i: (i, 0)), pl.BlockSpec((1, 1, tile), lambda i: (i, 0, 0))],
            compiler_params=pltpu.CompilerParams(vmem_limit_bytes=24 * 1024 * 1024),
            name='softmax',
        )(scores, allowed_valid.reshape(1, list_len), target_pos.reshape(rows_dev // tile, 1, tile))
        return probs, logp.reshape(rows_dev)

    row_spec = P(('rep', 'vocab'))
    mat_spec = P(('rep', 'vocab'), None)
    return jax.shard_map(device_step, mesh=mesh, in_specs=(mat_spec, P('vocab', None), P('rep'), P('rep'), row_spec), out_specs=(mat_spec, row_spec), check_vma=False)
```

```python
import functools

import jax
import jax.numpy as jnp
from jax import lax
from jax.experimental import pallas as pl
from jax.experimental.pallas import tpu as pltpu
from jax.sharding import PartitionSpec as P

INV_TEMP = 1.25
MESH = pl.DeviceIdType.MESH
CHUNK = 64
LAG = 2
GATHER = 32
PACK_BITS = 1
PACK = 1 << PACK_BITS
SCORED = 128
PIECES = 2
STAGES = 6
CUT = 768


def gather_kernel(shards, base_ref, local_ref, w_ref, gbuf_ref, stage, pick, in_sem):
    v = lax.axis_index('vocab')
    chip = v // 2

    def span(k):
        at = k * (shards + 1)
        first = base_ref[at + v]
        count = base_ref[at + v + 1] - first
        slot0 = first - base_ref[at + 2 * chip]
        block0 = slot0 // GATHER
        blocks = jnp.where(count > 0, (slot0 + count + GATHER - 1) // GATHER - block0, 0)
        return first, slot0, block0, blocks

    spans = [span(0), span(1)]
    total = spans[0][3] + spans[1][3]

    def where_is(t):
        second = t >= spans[0][3]
        first, slot0, block0 = [jnp.where(second, spans[1][i], spans[0][i]) for i in range(3)]
        k = jnp.where(second, 1, 0)
        block = block0 + jnp.where(second, t - spans[0][3], t)
        return k, block, first - slot0 + block * GATHER

    def row_copy(group, s, b):
        return pltpu.make_async_copy(
            w_ref.at[pl.ds(pl.multiple_of(group * PACK, PACK), PACK), :],
            stage.at[b, s],
            in_sem.at[b])

    lane = lax.broadcasted_iota(jnp.int32, (1, GATHER * PACK), 1)

    def issue(t, b):
        k, _, src = where_is(t)
        for s in range(GATHER):
            local = local_ref[k, src + s]
            group = lax.shift_right_logical(local, PACK_BITS)
            row_copy(group, s, b).start()
            pick[b, pl.ds(s, 1), :] = jnp.where(lane == s * PACK + (local & (PACK - 1)), 1.0, 0.0)

    def begin(t, carry):
        issue(t, t)
        return carry

    def wait_stage(b):
        pltpu.make_async_copy(stage.at[b], stage.at[b], in_sem.at[b]).wait()

    def step(t, carry):
        b = lax.rem(t, STAGES)

        @pl.when(t + STAGES - 1 < total)
        def _():
            issue(t + STAGES - 1, lax.rem(t + STAGES - 1, STAGES))

        wait_stage(b)
        k, block, _ = where_is(t)
        gbuf_ref[k, pl.ds(pl.multiple_of(block * GATHER, GATHER), GATHER), :] = jnp.dot(
            pick[b].astype(jnp.bfloat16), stage[b].reshape(GATHER * PACK, stage.shape[3]),
            preferred_element_type=jnp.float32).astype(gbuf_ref.dtype)
        return carry

    lax.fori_loop(0, jnp.minimum(total, STAGES - 1), begin, 0)
    lax.fori_loop(0, total, step, 0)


def ring_kernel(shards, base_ref, rank_ref, hid, gbuf_ref, out_ref,
                other, land, merged, theirs, slot_of, shift, older, newer,
                other_send, other_recv, ring_send, ring_recv, pair_send, pair_recv):
    chips = shards // 2
    half = gbuf_ref.shape[1]
    lag_rows = LAG * CHUNK
    n_own = half // CHUNK
    n_wire = n_own + (chips - 2) * LAG
    n_all = n_own + (chips - 1) * LAG
    max_delay = half // CHUNK + 1
    group = SCORED // CHUNK
    pad = -n_all % group
    gap = group // PIECES
    final = n_all - 1 - group + gap
    depth = hid.shape[1]
    v = lax.axis_index('vocab')
    core = lax.rem(v, 2)
    chip = v // 2
    partner = chip * 2 + 1 - core
    ahead = lax.rem(chip + 2 * core - 1 + chips, chips) * 2 + core
    behind = lax.rem(chip - 2 * core + 1 + chips, chips) * 2 + core

    barrier = pltpu.get_barrier_semaphore()
    for peer in (partner, ahead, behind):
        pl.semaphore_signal(barrier, inc=1, device_id={'vocab': peer}, device_id_type=MESH)

    def rows(e, n=CHUNK):
        return pl.ds(pl.multiple_of(e * CHUNK, CHUNK), n)

    def other_copy(e):
        return pltpu.make_async_remote_copy(
            src_ref=gbuf_ref.at[1 - core, rows(e), :], dst_ref=other.at[rows(e), :],
            send_sem=other_send.at[e], recv_sem=other_recv.at[e], device_id={'vocab': partner}, device_id_type=MESH)

    def ring_copy(e):
        return pltpu.make_async_remote_copy(
            src_ref=merged.at[rows(e + pad), :], dst_ref=land.at[rows(e), :],
            send_sem=ring_send.at[e], recv_sem=ring_recv.at[e], device_id={'vocab': ahead}, device_id_type=MESH)

    def pair_copy(e):
        return pltpu.make_async_remote_copy(
            src_ref=merged.at[rows(e + pad), :], dst_ref=theirs.at[rows(e + pad), :],
            send_sem=pair_send.at[e], recv_sem=pair_recv.at[e], device_id={'vocab': partner}, device_id_type=MESH)

    def base(k, w):
        return base_ref[k * (shards + 1) + w]

    pl.semaphore_wait(barrier, 3)
    ahead_of_use = 3
    for e in range(ahead_of_use):
        other_copy(e).start()

    for k in range(2):
        rank = rank_ref[pl.ds(k, 1), :]
        slots = jnp.zeros_like(rank)
        passed = jnp.int32(0)
        for hop in range(chips):
            owner = lax.rem(chip - (2 * k - 1) * hop + chips, chips)
            low, high = base(k, 2 * owner), base(k, 2 * owner + 2)
            slots += jnp.where((rank >= low) & (rank < high), rank + (passed - low), 0)
            passed += jnp.maximum(high - low, lag_rows)
        slot_of[k] = slots + pad * CHUNK
    if pad:
        merged[pl.ds(0, pad * CHUNK), :] = jnp.zeros((pad * CHUNK, depth), merged.dtype)
        theirs[pl.ds(0, pad * CHUNK), :] = jnp.zeros((pad * CHUNK, depth), theirs.dtype)
    older[...] = jnp.zeros_like(older)
    newer[...] = jnp.zeros_like(newer)

    chip_low = base(core, 2 * chip)
    own_pad = jnp.maximum(base(core, 2 * chip + 2) - chip_low, lag_rows)
    delay = (own_pad + CHUNK - 1) // CHUNK
    row = lax.broadcasted_iota(jnp.int32, (CHUNK, 2 * CHUNK), 0)
    col = lax.broadcasted_iota(jnp.int32, (CHUNK, 2 * CHUNK), 1)
    shift[...] = jnp.where(col == row + delay * CHUNK - own_pad, 1.0, 0.0).astype(jnp.bfloat16)
    mine_low = base(core, v) - chip_low
    mine_high = base(core, v + 1) - chip_low
    other_low = base(core, partner) - chip_low
    other_high = base(core, partner + 1) - chip_low

    def move(k, s, p, at, n):
        top = s.astype(jnp.bfloat16)
        rest = s - top.astype(jnp.float32)
        mid = rest.astype(jnp.bfloat16)
        low = (rest - mid.astype(jnp.float32)).astype(jnp.bfloat16)
        slot = lax.broadcasted_iota(jnp.int32, (SCORED, half), 0) + p * SCORED
        place = jnp.where(slot == slot_of[k], 1.0, 0.0).astype(jnp.bfloat16)
        moved = jnp.dot(jnp.concatenate([top, mid, low], axis=1), jnp.concatenate([place] * 3, axis=0),
                        preferred_element_type=jnp.float32)
        spot = (pl.ds(at, n), pl.ds(pl.multiple_of(k * half, half), half))
        out_ref[spot] = out_ref[spot] + moved

    def group_rows(p):
        return pl.ds(pl.multiple_of(p * SCORED, SCORED), SCORED)

    def against(at, n, part):
        return lax.dot_general(hid[pl.ds(at, n), :], part, (((1,), (1,)), ((), ())), preferred_element_type=jnp.float32) * INV_TEMP

    n_rows = hid.shape[0]

    def score(p, at, n):
        s = against(at, n, jnp.concatenate([merged[group_rows(p), :], theirs[group_rows(p), :]], axis=0))
        move(core, s[:, :SCORED], p, at, n)
        move(1 - core, s[:, SCORED:], p, at, n)

    def wait_theirs(p):
        for j in range(group):
            at = p * group + j - pad

            @pl.when(at >= 0)
            def _():
                pair_copy(at).wait_recv()

    def step(e, carry):
        @pl.when(e + ahead_of_use < n_own)
        def _():
            other_copy(e + ahead_of_use).start()

        @pl.when(e < n_own)
        def _():
            other_copy(e).wait_recv()

        @pl.when(e >= LAG)
        def _():
            ring_copy(e - LAG).wait_recv()
            for cut in range(depth // CUT):
                cols = pl.ds(cut * CUT, CUT)
                fresh = land[rows(e - LAG), cols]
                older[:, cols] = jnp.where(delay == LAG, fresh, older[:, cols])
                newer[:, cols] = jnp.where(delay == LAG + 1, fresh, newer[:, cols])

        slot = lax.broadcasted_iota(jnp.int32, (CHUNK, 1), 0) + e * CHUNK
        is_mine = (slot >= mine_low) & (slot < mine_high)
        is_other = (slot >= other_low) & (slot < other_high)
        e_own = jnp.minimum(e, n_own - 1)
        zero = jnp.zeros((), jnp.float32)
        for cut in range(depth // CUT):
            cols = pl.ds(cut * CUT, CUT)
            first, second = older[:, cols], newer[:, cols]
            older[:, cols] = second
            forward = jnp.dot(shift[...], jnp.concatenate([first, second], axis=0), preferred_element_type=jnp.float32)
            from_mine = jnp.where(is_mine, gbuf_ref[core, rows(e_own), cols].astype(jnp.float32), zero)
            from_other = jnp.where(is_other, other[rows(e_own), cols].astype(jnp.float32), zero)
            merged[rows(e + pad), cols] = (from_mine + from_other + forward).astype(jnp.bfloat16)

        @pl.when(e < n_wire)
        def _():
            ring_copy(e).start()

        pair_copy(e).start()

        for cut in range(depth // CUT):
            cols = pl.ds(cut * CUT, CUT)

            def pick(c, acc):
                return jnp.where(c == e + 2 - delay, land[rows(c), cols], acc)

            newer[:, cols] = lax.fori_loop(jnp.maximum(e + 2 - max_delay, 0), e - LAG + 1, pick,
                                           jnp.zeros((CHUNK, CUT), land.dtype))

        @pl.when(e == 0)
        def _():
            out_ref[...] = jnp.zeros_like(out_ref)

        since = e - (group - 1 - pad)

        @pl.when((since >= gap) & (lax.rem(since, gap) == 0) & (e <= final))
        def _():
            p = (since // gap - 1) // PIECES
            piece = lax.rem(since // gap - 1, PIECES)

            @pl.when(piece == 0)
            def _():
                wait_theirs(p)

            def one(i, c):
                score(p, pl.multiple_of(i * (n_rows // PIECES), n_rows // PIECES), n_rows // PIECES)
                return c

            lax.fori_loop(piece, jnp.where(e == final, PIECES, piece + 1), one, 0)

        return carry

    lax.fori_loop(0, n_all, step, 0)

    last = (n_all + pad) // group - 1
    wait_theirs(last)

    def tail(i, c):
        score(last, pl.multiple_of(i * (n_rows // PIECES), n_rows // PIECES), n_rows // PIECES)
        return c

    lax.fori_loop(0, PIECES, tail, 0)

    def finish(e, c):
        @pl.when(e < n_own)
        def _():
            other_copy(e).wait_send()

        @pl.when(e < n_wire)
        def _():
            ring_copy(e).wait_send()

        pair_copy(e).wait_send()
        return c

    lax.fori_loop(0, n_all, finish, 0)


def softmax_kernel(s_ref, valid_ref, target_ref, probs_ref, logp_ref):
    n = probs_ref.shape[0]
    s = s_ref[pl.ds(pl.multiple_of(pl.program_id(0) * n, n), n), :]
    eye = lax.broadcasted_iota(jnp.int32, (n, n), 0) == lax.broadcasted_iota(jnp.int32, (n, n), 1)
    target = jnp.sum(jnp.where(eye, target_ref[0], 0), axis=1, keepdims=True)
    masked = jnp.where(valid_ref[...] > 0, s, -jnp.inf)
    top = jnp.max(masked, axis=1, keepdims=True)
    power = jnp.exp(masked - top)
    total = jnp.sum(power, axis=1, keepdims=True)
    probs_ref[...] = power * (1.0 / total)
    lane = lax.broadcasted_iota(jnp.int32, s.shape, 1)
    picked = jnp.sum(jnp.where(lane == target, s, 0.0), axis=1, keepdims=True)
    logp = picked - (jnp.log(total) + top)
    logp_ref[0] = jnp.sum(jnp.where(eye, logp, 0.0), axis=0, keepdims=True)


def solution(mesh):
    shards = mesh.shape['vocab']

    def device_step(hidden, w_head, allowed_ids, allowed_valid, target_pos):
        list_len = allowed_ids.shape[0]
        half = list_len // 2
        vocab_local, depth = w_head.shape
        rows_dev = hidden.shape[0]
        chips = shards // 2
        ids = allowed_ids.reshape(2, half)
        rank = jnp.sum((ids[:, :, None] < ids[:, None, :]).astype(jnp.int32), axis=1)
        at = lax.broadcasted_iota(jnp.int32, (2, half + GATHER, half), 1)
        sorted_ids = jnp.sum(jnp.where(rank[:, None, :] == at, ids[:, None, :], 0), axis=2)
        local = jnp.clip(sorted_ids - lax.axis_index('vocab') * vocab_local, 0, vocab_local - 1)
        edges = lax.broadcasted_iota(jnp.int32, (2, shards + 1, half), 1) * vocab_local
        base = jnp.sum((ids[:, None, :] < edges).astype(jnp.int32).reshape(2 * (shards + 1), half), axis=1)

        gbuf = pl.pallas_call(
            functools.partial(gather_kernel, shards),
            out_shape=jax.ShapeDtypeStruct((2, half, depth), w_head.dtype),
            in_specs=[pl.BlockSpec(memory_space=pltpu.SMEM), pl.BlockSpec(memory_space=pltpu.SMEM), pl.BlockSpec(memory_space=pl.ANY)],
            out_specs=pl.BlockSpec(memory_space=pltpu.VMEM),
            scratch_shapes=[
                pltpu.VMEM((STAGES, GATHER, PACK, depth), w_head.dtype),
                pltpu.VMEM((STAGES, GATHER, GATHER * PACK), jnp.float32),
                pltpu.SemaphoreType.DMA((STAGES,)),
            ],
            compiler_params=pltpu.CompilerParams(vmem_limit_bytes=20 * 1024 * 1024),
            name='gather_rows',
        )(base, local, w_head)

        n_own = half // CHUNK
        n_wire = n_own + (chips - 2) * LAG
        n_all = n_own + (chips - 1) * LAG
        scores = pl.pallas_call(
            functools.partial(ring_kernel, shards),
            out_shape=jax.ShapeDtypeStruct((rows_dev, list_len), jnp.float32),
            in_specs=[pl.BlockSpec(memory_space=pltpu.SMEM), pl.BlockSpec(memory_space=pltpu.VMEM),
                      pl.BlockSpec(memory_space=pltpu.VMEM), pl.BlockSpec(memory_space=pltpu.VMEM)],
            out_specs=pl.BlockSpec(memory_space=pltpu.VMEM),
            scratch_shapes=[
                pltpu.VMEM((half, depth), w_head.dtype),
                pltpu.VMEM((n_wire * CHUNK, depth), w_head.dtype),
                pltpu.VMEM((pl.cdiv(n_all * CHUNK, SCORED) * SCORED, depth), w_head.dtype),
                pltpu.VMEM((pl.cdiv(n_all * CHUNK, SCORED) * SCORED, depth), w_head.dtype),
                pltpu.VMEM((2, 1, half), jnp.int32),
                pltpu.VMEM((CHUNK, 2 * CHUNK), jnp.bfloat16),
                pltpu.VMEM((CHUNK, depth), w_head.dtype),
                pltpu.VMEM((CHUNK, depth), w_head.dtype),
                pltpu.SemaphoreType.DMA((n_own,)),
                pltpu.SemaphoreType.DMA((n_own,)),
                pltpu.SemaphoreType.DMA((n_wire,)),
                pltpu.SemaphoreType.DMA((n_wire,)),
                pltpu.SemaphoreType.DMA((n_all,)),
                pltpu.SemaphoreType.DMA((n_all,)),
            ],
            compiler_params=pltpu.CompilerParams(collective_id=0, has_side_effects=True, vmem_limit_bytes=34 * 1024 * 1024),
            name='ring_scores',
        )(base, rank, hidden, gbuf)

        tile = 256
        probs, logp = pl.pallas_call(
            softmax_kernel,
            grid=(rows_dev // tile,),
            out_shape=[jax.ShapeDtypeStruct((rows_dev, list_len), jnp.float32), jax.ShapeDtypeStruct((rows_dev // tile, 1, tile), jnp.float32)],
            in_specs=[pl.BlockSpec(memory_space=pltpu.VMEM), pl.BlockSpec((1, list_len), lambda i: (0, 0)),
                      pl.BlockSpec((1, 1, tile), lambda i: (i, 0, 0))],
            out_specs=[pl.BlockSpec((tile, list_len), lambda i: (i, 0)), pl.BlockSpec((1, 1, tile), lambda i: (i, 0, 0))],
            compiler_params=pltpu.CompilerParams(vmem_limit_bytes=24 * 1024 * 1024),
            name='softmax',
        )(scores, allowed_valid.reshape(1, list_len), target_pos.reshape(rows_dev // tile, 1, tile))
        return probs, logp.reshape(rows_dev)

    row_spec = P(('rep', 'vocab'))
    mat_spec = P(('rep', 'vocab'), None)
    return jax.shard_map(device_step, mesh=mesh, in_specs=(mat_spec, P('vocab', None), P('rep'), P('rep'), row_spec), out_specs=(mat_spec, row_spec), check_vma=False)
```

```python
import functools

import jax
import jax.numpy as jnp
from jax import lax
from jax.experimental import pallas as pl
from jax.experimental.pallas import tpu as pltpu
from jax.sharding import PartitionSpec as P

INV_TEMP = 1.25
MESH = pl.DeviceIdType.MESH
CHUNK = 64
LAG = 2
GATHER = 32
PACK_BITS = 1
PACK = 1 << PACK_BITS
SCORED = 128
PIECES = 2
STAGES = 6
CUT = 768


def gather_kernel(shards, base_ref, local_ref, w_ref, gbuf_ref, stage, pick, in_sem):
    v = lax.axis_index('vocab')
    chip = v // 2

    def span(k):
        at = k * (shards + 1)
        first = base_ref[at + v]
        count = base_ref[at + v + 1] - first
        slot0 = first - base_ref[at + 2 * chip]
        block0 = slot0 // GATHER
        blocks = jnp.where(count > 0, (slot0 + count + GATHER - 1) // GATHER - block0, 0)
        return first, slot0, block0, blocks

    spans = [span(0), span(1)]
    total = spans[0][3] + spans[1][3]

    def where_is(t):
        second = t >= spans[0][3]
        first, slot0, block0 = [jnp.where(second, spans[1][i], spans[0][i]) for i in range(3)]
        k = jnp.where(second, 1, 0)
        block = block0 + jnp.where(second, t - spans[0][3], t)
        return k, block, first - slot0 + block * GATHER

    def row_copy(group, s, b):
        return pltpu.make_async_copy(
            w_ref.at[pl.ds(pl.multiple_of(group * PACK, PACK), PACK), :],
            stage.at[b, s],
            in_sem.at[b])

    lane = lax.broadcasted_iota(jnp.int32, (1, GATHER * PACK), 1)

    def issue(t, b):
        k, _, src = where_is(t)
        for s in range(GATHER):
            local = local_ref[k, src + s]
            group = lax.shift_right_logical(local, PACK_BITS)
            row_copy(group, s, b).start()
            pick[b, pl.ds(s, 1), :] = jnp.where(lane == s * PACK + (local & (PACK - 1)), 1.0, 0.0)

    def begin(t, carry):
        issue(t, t)
        return carry

    def wait_stage(b):
        pltpu.make_async_copy(stage.at[b], stage.at[b], in_sem.at[b]).wait()

    def step(t, carry):
        b = lax.rem(t, STAGES)

        @pl.when(t + STAGES - 1 < total)
        def _():
            issue(t + STAGES - 1, lax.rem(t + STAGES - 1, STAGES))

        wait_stage(b)
        k, block, _ = where_is(t)
        gbuf_ref[k, pl.ds(pl.multiple_of(block * GATHER, GATHER), GATHER), :] = jnp.dot(
            pick[b].astype(jnp.bfloat16), stage[b].reshape(GATHER * PACK, stage.shape[3]),
            preferred_element_type=jnp.float32).astype(gbuf_ref.dtype)
        return carry

    lax.fori_loop(0, jnp.minimum(total, STAGES - 1), begin, 0)
    lax.fori_loop(0, total, step, 0)


def ring_kernel(shards, base_ref, rank_ref, hid, gbuf_ref, out_ref,
                other, land, merged, theirs, slot_of, shift, older, newer,
                other_send, other_recv, ring_send, ring_recv, pair_send, pair_recv):
    chips = shards // 2
    half = gbuf_ref.shape[1]
    lag_rows = LAG * CHUNK
    n_own = half // CHUNK
    n_wire = n_own + (chips - 2) * LAG
    n_all = n_own + (chips - 1) * LAG
    max_delay = half // CHUNK + 1
    group = SCORED // CHUNK
    pad = -n_all % group
    gap = group // PIECES
    final = n_all - 1 - group + gap
    depth = hid.shape[1]
    v = lax.axis_index('vocab')
    core = lax.rem(v, 2)
    chip = v // 2
    partner = chip * 2 + 1 - core
    ahead = lax.rem(chip + 2 * core - 1 + chips, chips) * 2 + core
    behind = lax.rem(chip - 2 * core + 1 + chips, chips) * 2 + core

    barrier = pltpu.get_barrier_semaphore()
    for peer in (partner, ahead, behind):
        pl.semaphore_signal(barrier, inc=1, device_id={'vocab': peer}, device_id_type=MESH)

    def rows(e, n=CHUNK):
        return pl.ds(pl.multiple_of(e * CHUNK, CHUNK), n)

    def other_copy(e):
        return pltpu.make_async_remote_copy(
            src_ref=gbuf_ref.at[1 - core, rows(e), :], dst_ref=other.at[rows(e), :],
            send_sem=other_send.at[e], recv_sem=other_recv.at[e], device_id={'vocab': partner}, device_id_type=MESH)

    def ring_copy(e):
        return pltpu.make_async_remote_copy(
            src_ref=merged.at[rows(e + pad), :], dst_ref=land.at[rows(e), :],
            send_sem=ring_send.at[e], recv_sem=ring_recv.at[e], device_id={'vocab': ahead}, device_id_type=MESH)

    def pair_copy(e):
        return pltpu.make_async_remote_copy(
            src_ref=merged.at[rows(e + pad), :], dst_ref=theirs.at[rows(e + pad), :],
            send_sem=pair_send.at[e], recv_sem=pair_recv.at[e], device_id={'vocab': partner}, device_id_type=MESH)

    def base(k, w):
        return base_ref[k * (shards + 1) + w]

    pl.semaphore_wait(barrier, 3)
    ahead_of_use = 3
    for e in range(ahead_of_use):
        other_copy(e).start()

    for k in range(2):
        rank = rank_ref[pl.ds(k, 1), :]
        slots = jnp.zeros_like(rank)
        passed = jnp.int32(0)
        for hop in range(chips):
            owner = lax.rem(chip - (2 * k - 1) * hop + chips, chips)
            low, high = base(k, 2 * owner), base(k, 2 * owner + 2)
            slots += jnp.where((rank >= low) & (rank < high), rank + (passed - low), 0)
            passed += jnp.maximum(high - low, lag_rows)
        slot_of[k] = slots + pad * CHUNK
    if pad:
        merged[pl.ds(0, pad * CHUNK), :] = jnp.zeros((pad * CHUNK, depth), merged.dtype)
        theirs[pl.ds(0, pad * CHUNK), :] = jnp.zeros((pad * CHUNK, depth), theirs.dtype)
    older[...] = jnp.zeros_like(older)
    newer[...] = jnp.zeros_like(newer)

    chip_low = base(core, 2 * chip)
    own_pad = jnp.maximum(base(core, 2 * chip + 2) - chip_low, lag_rows)
    delay = (own_pad + CHUNK - 1) // CHUNK
    row = lax.broadcasted_iota(jnp.int32, (CHUNK, 2 * CHUNK), 0)
    col = lax.broadcasted_iota(jnp.int32, (CHUNK, 2 * CHUNK), 1)
    shift[...] = jnp.where(col == row + delay * CHUNK - own_pad, 1.0, 0.0).astype(jnp.bfloat16)
    mine_low = base(core, v) - chip_low
    mine_high = base(core, v + 1) - chip_low
    other_low = base(core, partner) - chip_low
    other_high = base(core, partner + 1) - chip_low

    def move(k, s, p, at, n):
        top = s.astype(jnp.bfloat16)
        rest = s - top.astype(jnp.float32)
        mid = rest.astype(jnp.bfloat16)
        low = (rest - mid.astype(jnp.float32)).astype(jnp.bfloat16)
        slot = lax.broadcasted_iota(jnp.int32, (SCORED, half), 0) + p * SCORED
        place = jnp.where(slot == slot_of[k], 1.0, 0.0).astype(jnp.bfloat16)
        moved = jnp.dot(jnp.concatenate([top, mid, low], axis=1), jnp.concatenate([place] * 3, axis=0),
                        preferred_element_type=jnp.float32)
        spot = (pl.ds(at, n), pl.ds(pl.multiple_of(k * half, half), half))
        out_ref[spot] = out_ref[spot] + moved

    def group_rows(p):
        return pl.ds(pl.multiple_of(p * SCORED, SCORED), SCORED)

    def against(at, n, part):
        return lax.dot_general(hid[pl.ds(at, n), :], part, (((1,), (1,)), ((), ())), preferred_element_type=jnp.float32) * INV_TEMP

    n_rows = hid.shape[0]

    def score(p, at, n):
        s = against(at, n, jnp.concatenate([merged[group_rows(p), :], theirs[group_rows(p), :]], axis=0))
        move(core, s[:, :SCORED], p, at, n)
        move(1 - core, s[:, SCORED:], p, at, n)

    def wait_theirs(p):
        for j in range(group):
            at = p * group + j - pad

            @pl.when(at >= 0)
            def _():
                pair_copy(at).wait_recv()

    def step(e, carry):
        @pl.when(e < n_own)
        def _():
            other_copy(e).wait_recv()

        @pl.when(e >= LAG)
        def _():
            ring_copy(e - LAG).wait_recv()
            for cut in range(depth // CUT):
                cols = pl.ds(cut * CUT, CUT)
                fresh = land[rows(e - LAG), cols]
                older[:, cols] = jnp.where(delay == LAG, fresh, older[:, cols])
                newer[:, cols] = jnp.where(delay == LAG + 1, fresh, newer[:, cols])

        slot = lax.broadcasted_iota(jnp.int32, (CHUNK, 1), 0) + e * CHUNK
        is_mine = (slot >= mine_low) & (slot < mine_high)
        is_other = (slot >= other_low) & (slot < other_high)
        e_own = jnp.minimum(e, n_own - 1)
        zero = jnp.zeros((), jnp.float32)
        for cut in range(depth // CUT):
            cols = pl.ds(cut * CUT, CUT)
            first, second = older[:, cols], newer[:, cols]
            older[:, cols] = second
            forward = jnp.dot(shift[...], jnp.concatenate([first, second], axis=0), preferred_element_type=jnp.float32)
            from_mine = jnp.where(is_mine, gbuf_ref[core, rows(e_own), cols].astype(jnp.float32), zero)
            from_other = jnp.where(is_other, other[rows(e_own), cols].astype(jnp.float32), zero)
            merged[rows(e + pad), cols] = (from_mine + from_other + forward).astype(jnp.bfloat16)

        @pl.when(e < n_wire)
        def _():
            ring_copy(e).start()

        @pl.when(e + ahead_of_use < n_own)
        def _():
            other_copy(e + ahead_of_use).start()

        pair_copy(e).start()

        for cut in range(depth // CUT):
            cols = pl.ds(cut * CUT, CUT)

            def pick(c, acc):
                return jnp.where(c == e + 2 - delay, land[rows(c), cols], acc)

            newer[:, cols] = lax.fori_loop(jnp.maximum(e + 2 - max_delay, 0), e - LAG + 1, pick,
                                           jnp.zeros((CHUNK, CUT), land.dtype))

        @pl.when(e == 0)
        def _():
            out_ref[...] = jnp.zeros_like(out_ref)

        since = e - (group - 1 - pad)

        @pl.when((since >= gap) & (lax.rem(since, gap) == 0) & (e <= final))
        def _():
            p = (since // gap - 1) // PIECES
            piece = lax.rem(since // gap - 1, PIECES)

            @pl.when(piece == 0)
            def _():
                wait_theirs(p)

            def one(i, c):
                score(p, pl.multiple_of(i * (n_rows // PIECES), n_rows // PIECES), n_rows // PIECES)
                return c

            lax.fori_loop(piece, jnp.where(e == final, PIECES, piece + 1), one, 0)

        return carry

    lax.fori_loop(0, n_all, step, 0)

    last = (n_all + pad) // group - 1
    wait_theirs(last)

    def tail(i, c):
        score(last, pl.multiple_of(i * (n_rows // PIECES), n_rows // PIECES), n_rows // PIECES)
        return c

    lax.fori_loop(0, PIECES, tail, 0)

    def finish(e, c):
        @pl.when(e < n_own)
        def _():
            other_copy(e).wait_send()

        @pl.when(e < n_wire)
        def _():
            ring_copy(e).wait_send()

        pair_copy(e).wait_send()
        return c

    lax.fori_loop(0, n_all, finish, 0)


def softmax_kernel(s_ref, valid_ref, target_ref, probs_ref, logp_ref):
    n = probs_ref.shape[0]
    s = s_ref[pl.ds(pl.multiple_of(pl.program_id(0) * n, n), n), :]
    eye = lax.broadcasted_iota(jnp.int32, (n, n), 0) == lax.broadcasted_iota(jnp.int32, (n, n), 1)
    target = jnp.sum(jnp.where(eye, target_ref[0], 0), axis=1, keepdims=True)
    masked = jnp.where(valid_ref[...] > 0, s, -jnp.inf)
    top = jnp.max(masked, axis=1, keepdims=True)
    power = jnp.exp(masked - top)
    total = jnp.sum(power, axis=1, keepdims=True)
    probs_ref[...] = power * (1.0 / total)
    lane = lax.broadcasted_iota(jnp.int32, s.shape, 1)
    picked = jnp.sum(jnp.where(lane == target, s, 0.0), axis=1, keepdims=True)
    logp = picked - (jnp.log(total) + top)
    logp_ref[0] = jnp.sum(jnp.where(eye, logp, 0.0), axis=0, keepdims=True)


def solution(mesh):
    shards = mesh.shape['vocab']

    def device_step(hidden, w_head, allowed_ids, allowed_valid, target_pos):
        list_len = allowed_ids.shape[0]
        half = list_len // 2
        vocab_local, depth = w_head.shape
        rows_dev = hidden.shape[0]
        chips = shards // 2
        ids = allowed_ids.reshape(2, half)
        rank = jnp.sum((ids[:, :, None] < ids[:, None, :]).astype(jnp.int32), axis=1)
        at = lax.broadcasted_iota(jnp.int32, (2, half + GATHER, half), 1)
        sorted_ids = jnp.sum(jnp.where(rank[:, None, :] == at, ids[:, None, :], 0), axis=2)
        local = jnp.clip(sorted_ids - lax.axis_index('vocab') * vocab_local, 0, vocab_local - 1)
        edges = lax.broadcasted_iota(jnp.int32, (2, shards + 1, half), 1) * vocab_local
        base = jnp.sum((ids[:, None, :] < edges).astype(jnp.int32).reshape(2 * (shards + 1), half), axis=1)

        gbuf = pl.pallas_call(
            functools.partial(gather_kernel, shards),
            out_shape=jax.ShapeDtypeStruct((2, half, depth), w_head.dtype),
            in_specs=[pl.BlockSpec(memory_space=pltpu.SMEM), pl.BlockSpec(memory_space=pltpu.SMEM), pl.BlockSpec(memory_space=pl.ANY)],
            out_specs=pl.BlockSpec(memory_space=pltpu.VMEM),
            scratch_shapes=[
                pltpu.VMEM((STAGES, GATHER, PACK, depth), w_head.dtype),
                pltpu.VMEM((STAGES, GATHER, GATHER * PACK), jnp.float32),
                pltpu.SemaphoreType.DMA((STAGES,)),
            ],
            compiler_params=pltpu.CompilerParams(vmem_limit_bytes=20 * 1024 * 1024),
            name='gather_rows',
        )(base, local, w_head)

        n_own = half // CHUNK
        n_wire = n_own + (chips - 2) * LAG
        n_all = n_own + (chips - 1) * LAG
        scores = pl.pallas_call(
            functools.partial(ring_kernel, shards),
            out_shape=jax.ShapeDtypeStruct((rows_dev, list_len), jnp.float32),
            in_specs=[pl.BlockSpec(memory_space=pltpu.SMEM), pl.BlockSpec(memory_space=pltpu.VMEM),
                      pl.BlockSpec(memory_space=pltpu.VMEM), pl.BlockSpec(memory_space=pltpu.VMEM)],
            out_specs=pl.BlockSpec(memory_space=pltpu.VMEM),
            scratch_shapes=[
                pltpu.VMEM((half, depth), w_head.dtype),
                pltpu.VMEM((n_wire * CHUNK, depth), w_head.dtype),
                pltpu.VMEM((pl.cdiv(n_all * CHUNK, SCORED) * SCORED, depth), w_head.dtype),
                pltpu.VMEM((pl.cdiv(n_all * CHUNK, SCORED) * SCORED, depth), w_head.dtype),
                pltpu.VMEM((2, 1, half), jnp.int32),
                pltpu.VMEM((CHUNK, 2 * CHUNK), jnp.bfloat16),
                pltpu.VMEM((CHUNK, depth), w_head.dtype),
                pltpu.VMEM((CHUNK, depth), w_head.dtype),
                pltpu.SemaphoreType.DMA((n_own,)),
                pltpu.SemaphoreType.DMA((n_own,)),
                pltpu.SemaphoreType.DMA((n_wire,)),
                pltpu.SemaphoreType.DMA((n_wire,)),
                pltpu.SemaphoreType.DMA((n_all,)),
                pltpu.SemaphoreType.DMA((n_all,)),
            ],
            compiler_params=pltpu.CompilerParams(collective_id=0, has_side_effects=True, vmem_limit_bytes=34 * 1024 * 1024),
            name='ring_scores',
        )(base, rank, hidden, gbuf)

        tile = 256
        probs, logp = pl.pallas_call(
            softmax_kernel,
            grid=(rows_dev // tile,),
            out_shape=[jax.ShapeDtypeStruct((rows_dev, list_len), jnp.float32), jax.ShapeDtypeStruct((rows_dev // tile, 1, tile), jnp.float32)],
            in_specs=[pl.BlockSpec(memory_space=pltpu.VMEM), pl.BlockSpec((1, list_len), lambda i: (0, 0)),
                      pl.BlockSpec((1, 1, tile), lambda i: (i, 0, 0))],
            out_specs=[pl.BlockSpec((tile, list_len), lambda i: (i, 0)), pl.BlockSpec((1, 1, tile), lambda i: (i, 0, 0))],
            compiler_params=pltpu.CompilerParams(vmem_limit_bytes=24 * 1024 * 1024),
            name='softmax',
        )(scores, allowed_valid.reshape(1, list_len), target_pos.reshape(rows_dev // tile, 1, tile))
        return probs, logp.reshape(rows_dev)

    row_spec = P(('rep', 'vocab'))
    mat_spec = P(('rep', 'vocab'), None)
    return jax.shard_map(device_step, mesh=mesh, in_specs=(mat_spec, P('vocab', None), P('rep'), P('rep'), row_spec), out_specs=(mat_spec, row_spec), check_vma=False)
```
